512 devices in a mesh: dp: 16 (over x_lo, y, core), vocab: 32 (over x_hi, z).
Axes of the slice: x: 4 (x_hi: 2, x_lo: 2; x = x_hi * 2 + x_lo), y: 4, z: 16, core: 2. Of those that a mesh axis runs over, the one named last changes fastest.
Arguments:
- student_hidden: bfloat16 [2048, 2048], P('dp', 'vocab'), may hold values from -210 to 210
- student_blocks: bfloat16 [32, 1024, 4864], P('vocab', 'dp'), may hold values from -0.375 to 0.375
- teacher_logits: bfloat16 [2048, 77824], P('dp', 'vocab'), may hold values from -16 to 308
- token_ids: int32 [2048], P('dp'), may hold values from 0 to 77823
- loss_mask: int32 [2048], P('dp'), may hold values from 0 to 1, as said below
Outputs:
- hidden_grad: bfloat16 [2048, 2048], P('dp', 'vocab')
- token_kl: float32 [2048], P('dp')
- sampled_logprob: float32 [2048], P('dp')
- loss: float32 [], replicated
The draws below stay inside these ranges and needn't reach their ends.
Inputs may be any that keep to these rules, and one draw needn't show every extreme that they name: `loss_mask`: in each block of 128 tokens the mask is 0 on a leading run of at most 64 tokens and 1 on the rest.
All inputs are finite; a program needn't handle non-finite values.
Results may differ from the reference program's by a relative error of at most 0.0047.
Values may be sent and summed in bfloat16 or wider, within the bound.
A program may use at most 64 MiB of HBM per device.

```python
import jax
import jax.numpy as jnp
from jax import lax

D = 2048
VT = 2432
TOK_DEV = 128
TOKENS = 2048
V = 77824
N_VOCAB = 32


def draw_student_hidden(key, part):
    first_key = jax.random.fold_in(key, 0)
    values = jnp.clip(jax.random.normal(first_key, (TOKENS, D), jnp.float32), -6.0, 6.0)
    return values.astype(jnp.bfloat16)


def draw_teacher_logits(key, part):
    first_key = jax.random.fold_in(key, 0)
    return jnp.clip(3.0 * jax.random.normal(first_key, (TOKENS, V), jnp.float32), -16.0, 16.0).astype(jnp.bfloat16)


def draw_loss_mask(key, part):
    blocks = TOKENS // TOK_DEV
    starts = jax.random.randint(key, (blocks, 1), 0, TOK_DEV // 2 + 1)
    position = jnp.arange(TOK_DEV, dtype=jnp.int32)[None, :]
    return (position >= starts).astype(jnp.int32).reshape(TOKENS)


def set_ends(result, key, least, top_value):
    longest = result.shape.index(max(result.shape))
    spots = []
    for shift in (0, 1):
        where = [jax.random.randint(jax.random.fold_in(key, axis), (), 0, length) for axis, length in enumerate(result.shape)]
        where[longest] = (where[longest] + shift) % result.shape[longest]
        spots.append(tuple(where))
    return result.at[spots[0]].set(least).at[spots[1]].set(top_value)


def levels(stream_key, shape, cuts, least, high):
    gain = 1.0
    for dim, blocks in cuts:
        steps = jax.random.uniform(jax.random.fold_in(jax.random.fold_in(stream_key, 6), dim), (blocks,), jnp.float32, least / len(cuts), high / len(cuts))
        gain = gain * jnp.repeat(jnp.exp(steps), shape[dim] // blocks).reshape((-1,) + (1,) * (len(shape) - 1 - dim))
    return gain


def noise(stream_key, shape, scale, most, cuts=(), kind=jnp.bfloat16):
    array = scale * jax.random.normal(stream_key, shape, jnp.float32)
    if cuts:
        array = array * levels(stream_key, shape, cuts, -0.22, 0.18)
    return jnp.clip(array, -most, most).astype(kind)


def setup_inputs(seed: int = 0) -> dict:
    key_of = jax.random.split(jax.random.key(seed), 6)
    return {
        "student_hidden": draw_student_hidden(jax.random.fold_in(key_of[5], 71), 0),
        "student_blocks": noise(key_of[1], (N_VOCAB, D // 2, 2 * VT), (D // 9) ** -0.5, 0.375, ((0, 32), (1, 16))),
        "teacher_logits": draw_teacher_logits(jax.random.fold_in(key_of[5], 71), 0),
        "token_ids": set_ends(jax.random.randint(key_of[3], (TOKENS,), 0, V), jax.random.fold_in(key_of[3], 1), 0, V - 1).astype(jnp.int32),
        "loss_mask": draw_loss_mask(jax.random.fold_in(key_of[5], 71), 0),
    }


def reference(student_hidden, student_blocks, teacher_logits, token_ids, loss_mask):
    shards = N_VOCAB // 2
    width = 2 * VT
    weight = student_blocks.reshape(shards, 2, D // 2, width).transpose(1, 2, 0, 3).reshape(D, shards * width)
    mask_total = jnp.sum(loss_mask.astype(jnp.float32))

    def block(inputs):
        hidden, teacher, ids, mask = inputs
        logits = jnp.dot(hidden, weight, preferred_element_type=jnp.float32)
        student_logp = jax.nn.log_softmax(logits, axis=-1)
        teacher_logp = jax.nn.log_softmax(teacher.astype(jnp.float32), axis=-1)
        teacher_prob = jnp.exp(teacher_logp)
        kl_rows = jnp.sum(teacher_prob * (teacher_logp - student_logp), axis=-1)
        sampled = jnp.take_along_axis(student_logp, ids.astype(jnp.int32)[:, None], axis=1)[:, 0]
        factor = mask.astype(jnp.float32) / mask_total
        dlogits = (factor[:, None] * (jnp.exp(student_logp) - teacher_prob)).astype(jnp.bfloat16)
        grads = lax.dot_general(dlogits, weight, (((1,), (1,)), ((), ())), preferred_element_type=jnp.float32)
        return grads.astype(jnp.bfloat16), kl_rows, sampled

    blocks = TOKENS // TOK_DEV
    grads, kl_rows, sampled = lax.map(block, (student_hidden.reshape(blocks, TOK_DEV, D), teacher_logits.reshape(blocks, TOK_DEV, V), token_ids.reshape(blocks, TOK_DEV), loss_mask.reshape(blocks, TOK_DEV)))
    token_kl = kl_rows.reshape(TOKENS)
    loss = jnp.sum(loss_mask.astype(jnp.float32) * token_kl) / mask_total
    return grads.reshape(TOKENS, D), token_kl, sampled.reshape(TOKENS), loss
```

```python
import jax
import jax.numpy as jnp
from jax import lax
from jax.experimental import pallas as pl
from jax.experimental.pallas import tpu as pltpu
from jax.sharding import PartitionSpec as P

F32 = jnp.float32
BF16 = jnp.bfloat16
D = 2048
VT = 2432
TOK = 128
R = 64
NT = VT // 128
NZ = 16
MESH = pl.DeviceIdType.MESH

XP, YP, YM, ZP, CP = range(5)


def kernel(
    hid_ref, blk_ref, tea_ref, ids_ref, mask_ref,
    grad_ref, kl_ref, samp_ref, loss_ref,
    w, ht, hg, acc, lt, tt, et, dl, stat, mrow, lrow, xsend, xrecv, own, zsend, zrecv,
    w_send, w_recv, d_send, d_recv, loc_sem, h_send, h_recv,
    s_send, s_recv, m_send, m_recv, l_send, l_recv, x_send, x_recv, z_send, z_recv,
):
    d = lax.axis_index("dp")
    v = lax.axis_index("vocab")
    xl, y, c = d // 8, (d // 2) % 4, d % 2
    xh, z = v // NZ, v % NZ
    h = v % 2

    def dev(dp, vocab):
        return {"dp": dp, "vocab": vocab}

    target = {
        XP: dev(d ^ 8, v),
        YP: dev(xl * 8 + ((y + 1) % 4) * 2 + c, v),
        YM: dev(xl * 8 + ((y + 3) % 4) * 2 + c, v),
        ZP: dev(d, v ^ 1),
        CP: dev(d ^ 1, v),
    }
    far = [8, 7, 9, 6, 10, 5, 11, 4, 12, 3, 13, 2, 14, 1, 15]

    barrier = pltpu.get_barrier_semaphore()
    for r in range(1, 32):
        pl.semaphore_signal(barrier, inc=1, device_id=dev(d, v ^ r), device_id_type=MESH)
    for r in range(1, 16):
        pl.semaphore_signal(barrier, inc=1, device_id=dev(d ^ r, v), device_id_type=MESH)
    pl.semaphore_wait(barrier, 46)

    started = []

    def send(src, dst, ssem, rsem, to):
        copy = pltpu.make_async_remote_copy(
            src_ref=src, dst_ref=dst, send_sem=ssem, recv_sem=rsem, device_id=to, device_id_type=MESH
        )
        copy.start()
        started.append(copy)

    def arrived(dst, sem):
        pltpu.make_async_copy(dst, dst, sem).wait()

    def rows_of(t, dx, dy, core, half=None):
        base = (h ^ t) * 1024 + R * ((xl ^ dx) * 8 + ((y + dy) % 4) * 2 + core)
        if half is None:
            return pl.ds(pl.multiple_of(base, R), R)
        return pl.ds(pl.multiple_of(base + 32 * half, 32), 32)

    counter = {"w": 0, "d": 0}

    def sem_index(t, dx, dy, half):
        base = (t * 2 + dx) * 5
        return base + (dy if dy < 2 else 2 + half if dy == 2 else 4)

    def pass_on(t, dx, dy, way, half=None, src=None):
        ref = w.at[rows_of(t, dx, dy, c, half)]
        if way == XP:
            at = (t, dx ^ 1, dy)
        elif way == YP:
            at = (t, dx, (dy + 3) % 4)
        elif way == YM:
            at = (t, dx, (dy + 1) % 4)
        k = counter["w"]
        counter["w"] += 1
        send(ref if src is None else src, ref, w_send.at[k], w_recv.at[sem_index(*at, half or 0)], target[way])

    def across(t, dx, dy, half=None, src=None):
        ref = w.at[rows_of(t, dx, dy, c, half)]
        k = counter["d"]
        counter["d"] += 1
        send(ref if src is None else src, ref, d_send.at[k], d_recv.at[sem_index(t, dx, dy, half or 0)], target[CP])

    def piece_in(t, dx, dy, half=None):
        arrived(w.at[rows_of(t, dx, dy, c, half)], w_recv.at[sem_index(t, dx, dy, half or 0)])

    def peer_in(t, dx):
        for dy in range(4):
            for half in (0, 1) if dy == 2 else (None,):
                arrived(w.at[rows_of(t, dx, dy, 1 - c, half)], d_recv.at[sem_index(t, dx, dy, half or 0)])

    near = blk_ref.at[:, pl.ds(pl.multiple_of(h * VT, 128), VT)]
    away = blk_ref.at[:, pl.ds(pl.multiple_of((1 - h) * VT, 128), VT)]
    shard = jnp.concatenate([hid_ref[...].astype(F32), jnp.zeros((TOK, 128 - R), F32)], axis=1)
    mine = pl.ds(pl.multiple_of(xh * R, R), R)
    theirs = pl.ds(pl.multiple_of((1 - xh) * R, R), R)
    ht[z, mine, :] = shard.T[:R].astype(BF16)
    mrow[d] = mask_ref[...].astype(F32)
    send(ht.at[z, mine], ht.at[z, mine], h_send.at[15], h_recv.at[1], dev(d, v ^ NZ))
    send(away, w.at[pl.ds(pl.multiple_of(h * 1024 + R * d, R), R)], w_send.at[19], w_recv.at[sem_index(1, 0, 0, 0)], target[ZP])
    pass_on(0, 0, 0, XP, src=near)
    pass_on(0, 0, 0, YP, src=near)
    pass_on(0, 0, 0, YM, src=near)
    across(0, 0, 0, src=near)
    place = pltpu.make_async_copy(near, w.at[rows_of(0, 0, 0, c)], loc_sem)
    place.start()
    for r in range(1, 16):
        send(mrow.at[d], mrow.at[d], m_send.at[r - 1], m_recv, dev(d ^ r, v))

    def turn_teacher(j, top):
        at = pl.ds(pl.multiple_of(j * 128, 128), 128)
        block = tea_ref[:, at].astype(F32).T
        tt[at, :] = block
        return jnp.maximum(top, block.reshape(16, 8, 128).max(axis=0))

    top = lax.fori_loop(0, NT, turn_teacher, jnp.full((8, 128), -jnp.inf, F32))
    t_max = top.max(axis=0, keepdims=True)

    def exp_teacher(j, total):
        at = pl.ds(pl.multiple_of(j * 128, 128), 128)
        e = jnp.exp(tt[at, :] - t_max)
        et[at, :] = e
        return total + e.reshape(16, 8, 128).sum(axis=0)

    t_sum = lax.fori_loop(0, NT, exp_teacher, jnp.zeros((8, 128), F32)).sum(axis=0, keepdims=True)

    arrived(ht.at[z, theirs], h_recv.at[1])
    for i, k in enumerate(far):
        send(ht.at[z], ht.at[z], h_send.at[i], h_recv.at[0], dev(d, xh * NZ + (z + k) % NZ))

    piece_in(0, 0, 3)
    pass_on(0, 0, 3, YP, half=0)
    pass_on(0, 0, 3, XP)
    across(0, 0, 3)
    piece_in(0, 0, 1)
    pass_on(0, 0, 1, YM, half=1)
    across(0, 0, 1)
    piece_in(1, 0, 0)
    pass_on(1, 0, 0, XP)
    pass_on(1, 0, 0, YP)
    pass_on(1, 0, 0, YM)
    across(1, 0, 0)
    pass_on(0, 0, 1, XP)
    piece_in(0, 1, 0)
    across(0, 1, 0)
    for half in (0, 1):
        piece_in(0, 0, 2, half)
        pass_on(0, 0, 2, XP, half=half)
        across(0, 0, 2, half)
    piece_in(0, 1, 3)
    across(0, 1, 3)
    piece_in(1, 0, 3)
    pass_on(1, 0, 3, YP, half=0)
    across(1, 0, 3)
    piece_in(1, 0, 1)
    pass_on(1, 0, 1, YM, half=1)
    across(1, 0, 1)
    piece_in(1, 1, 0)
    pass_on(1, 1, 0, YP)
    pass_on(1, 1, 0, YM)
    across(1, 1, 0)
    for half in (0, 1):
        piece_in(1, 0, 2, half)
        across(1, 0, 2, half)

    arrived(ht.at[pl.ds(0, 15)], h_recv.at[0])
    for g in range(4):
        part = ht[8 * (g % 2) : 8 * (g % 2) + 8, (g // 2) * R : (g // 2) * R + R, :]
        hg[g] = part.reshape(512, TOK).astype(F32).T.astype(BF16)

    def multiply(t, dx, first):
        g = (h ^ t) * 2 + (xl ^ dx)
        rows = pl.ds(pl.multiple_of(g * 512, 512), 512)
        part = jnp.dot(hg[g], w[rows, :], preferred_element_type=F32)
        acc[...] = part if first else acc[...] + part

    place.wait()
    peer_in(0, 0)
    multiply(0, 0, True)
    piece_in(0, 1, 1)
    across(0, 1, 1)
    piece_in(1, 1, 3)
    pass_on(1, 1, 3, YP, half=0)
    across(1, 1, 3)
    piece_in(1, 1, 1)
    pass_on(1, 1, 1, YM, half=1)
    across(1, 1, 1)
    peer_in(1, 0)
    multiply(1, 0, False)
    for half in (0, 1):
        piece_in(1, 1, 2, half)
        across(1, 1, 2, half)
    for half in (0, 1):
        piece_in(0, 1, 2, half)
        across(0, 1, 2, half)
    peer_in(1, 1)
    multiply(1, 1, False)
    peer_in(0, 1)
    multiply(0, 1, False)

    ids = ids_ref[...]

    def turn_student(j, carry):
        top, hit = carry
        at = pl.ds(pl.multiple_of(j * 128, 128), 128)
        block = acc[:, at].T
        lt[at, :] = block
        column = lax.broadcasted_iota(jnp.int32, (128, 128), 0) + (v * VT + j * 128)
        found = jnp.where(column == ids, block, 0.0)
        return (
            jnp.maximum(top, block.reshape(16, 8, 128).max(axis=0)),
            hit + found.reshape(16, 8, 128).sum(axis=0),
        )

    zero8 = jnp.zeros((8, 128), F32)
    top, hit = lax.fori_loop(0, NT, turn_student, (jnp.full((8, 128), -jnp.inf, F32), zero8))
    s_max = top.max(axis=0, keepdims=True)

    def exp_student(j, carry):
        total, cross = carry
        at = pl.ds(pl.multiple_of(j * 128, 128), 128)
        s = lt[at, :]
        e = jnp.exp(s - s_max)
        x = et[at, :] * (tt[at, :] - s)
        lt[at, :] = e
        return total + e.reshape(16, 8, 128).sum(axis=0), cross + x.reshape(16, 8, 128).sum(axis=0)

    total, cross = lax.fori_loop(0, NT, exp_student, (zero8, zero8))
    s_sum = total.sum(axis=0, keepdims=True)
    x_sum = cross.sum(axis=0, keepdims=True)
    s_hit = hit.sum(axis=0, keepdims=True)
    stat[v] = jnp.concatenate([t_max, s_max, t_sum, x_sum, s_sum, s_hit, s_hit, s_hit], axis=0)

    k = 0
    for offset in far + [0]:
        for other in (1, 0):
            if other or offset:
                to = dev(d, (xh ^ other) * NZ + (z + offset) % NZ)
                send(stat.at[v], stat.at[v], s_send.at[k], s_recv, to)
                k += 1
    arrived(mrow.at[pl.ds(0, 15)], m_recv)
    count_row = mrow[0]
    for r in range(1, 16):
        count_row = count_row + mrow[r]
    count = jnp.sum(count_row, axis=1, keepdims=True)
    factor = mask_ref[...].astype(F32) / count
    arrived(stat.at[pl.ds(0, 31)], s_recv)
    tops = stat[0]
    for r in range(1, 32):
        tops = jnp.maximum(tops, stat[r])
    tops = tops[0:2]
    tz = xz = sz = hz = jnp.zeros((1, 128), F32)
    for r in range(32):
        one = stat[r]
        scale = jnp.exp(one[0:2] - tops)
        tz = tz + scale[0:1] * one[2:3]
        xz = xz + scale[0:1] * one[3:4]
        sz = sz + scale[1:2] * one[4:5]
        hz = hz + one[5:6]
    t_lse = tops[0:1] + jnp.log(tz)
    s_lse = tops[1:2] + jnp.log(sz)
    kl = xz / tz - t_lse + s_lse
    kl_ref[...] = kl
    samp_ref[...] = hz - s_lse
    lrow[d] = kl * mask_ref[...].astype(F32)
    for r in range(1, 16):
        send(lrow.at[d], lrow.at[d], l_send.at[r - 1], l_recv, dev(d ^ r, v))

    s_scale = factor * (jnp.exp(s_max - tops[1:2]) / sz)
    t_scale = factor * (jnp.exp(t_max - tops[0:1]) / tz)

    def make_dl(j, _):
        at = pl.ds(pl.multiple_of(j * 128, 128), 128)
        dl[at, :] = (lt[at, :] * s_scale - et[at, :] * t_scale).astype(BF16)
        return 0

    lax.fori_loop(0, NT, make_dl, 0)

    def quarter(half, q):
        rows = pl.ds(pl.multiple_of(half * 1024 + q * 256, 256), 256)
        return jnp.dot(w[rows, :], dl[...], preferred_element_type=F32)

    order = [(z // 4 + s) % 4 for s in (2, 1, 3, 0)]
    for i in range(4):
        xsend[i] = quarter(1 - xh, order[i]).astype(BF16)
        send(xsend.at[i], xrecv.at[i], x_send.at[i], x_recv.at[i], dev(d, v ^ NZ))
    for i in range(4):
        own[i] = quarter(xh, order[i])
    k = 0
    for i in range(4):
        arrived(xrecv.at[i], x_recv.at[i])
        both = own[i] + xrecv[i].astype(F32)
        own[i] = both
        zsend[i] = both.astype(BF16)
        for r in range(4) if i < 3 else (2, 3, 1):
            zt = order[i] * 4 + r if i < 3 else z ^ r
            piece = zsend.at[i, pl.ds(pl.multiple_of((zt % 4) * R, R), R)]
            send(piece, zrecv.at[z], z_send.at[k], z_recv, dev(d, xh * NZ + zt))
            k += 1

    arrived(lrow.at[pl.ds(0, 15)], l_recv)
    loss_row = lrow[0]
    for r in range(1, 16):
        loss_row = loss_row + lrow[r]
    loss_ref[...] = jnp.sum(loss_row, axis=1, keepdims=True) / count

    kept = own[3, pl.ds(pl.multiple_of((z % 4) * R, R), R), :]
    arrived(zrecv.at[pl.ds(0, 15)], z_recv)
    for r in range(1, 16):
        kept = kept + zrecv[z ^ r].astype(F32)
    turned = jnp.concatenate([kept, jnp.zeros((128 - R, TOK), F32)], axis=0).T
    grad_ref[...] = turned[:, :R].astype(BF16)
    for copy in started:
        copy.wait_send()


def on_device(hidden, blocks, teacher, ids, mask):
    vm = pl.BlockSpec(memory_space=pltpu.VMEM)
    dma = pltpu.SemaphoreType.DMA
    outs = pl.pallas_call(
        kernel,
        out_shape=(
            jax.ShapeDtypeStruct((TOK, R), BF16),
            jax.ShapeDtypeStruct((1, TOK), F32),
            jax.ShapeDtypeStruct((1, TOK), F32),
            jax.ShapeDtypeStruct((1, 1), F32),
        ),
        in_specs=[vm, pl.BlockSpec(memory_space=pl.ANY), vm, vm, vm],
        out_specs=(vm, vm, vm, vm),
        scratch_shapes=[
            pltpu.VMEM((D, VT), BF16),
            pltpu.VMEM((NZ, 2 * R, TOK), BF16),
            pltpu.VMEM((4, TOK, 512), BF16),
            pltpu.VMEM((TOK, VT), F32),
            pltpu.VMEM((VT, TOK), F32),
            pltpu.VMEM((VT, TOK), F32),
            pltpu.VMEM((VT, TOK), F32),
            pltpu.VMEM((VT, TOK), BF16),
            pltpu.VMEM((32, 8, TOK), F32),
            pltpu.VMEM((16, 1, TOK), F32),
            pltpu.VMEM((16, 1, TOK), F32),
            pltpu.VMEM((4, 256, TOK), BF16),
            pltpu.VMEM((4, 256, TOK), BF16),
            pltpu.VMEM((4, 256, TOK), F32),
            pltpu.VMEM((4, 256, TOK), BF16),
            pltpu.VMEM((NZ, R, TOK), BF16),
            dma((20,)), dma((20,)), dma((20,)), dma((20,)), dma, dma((16,)), dma((2,)),
            dma((31,)), dma, dma((15,)), dma, dma((15,)), dma, dma((4,)), dma((4,)), dma((15,)), dma,
        ],
        compiler_params=pltpu.CompilerParams(
            collective_id=0, has_side_effects=True, vmem_limit_bytes=60 * 1024 * 1024
        ),
    )(hidden, blocks.reshape(R, 2 * VT), teacher, ids.reshape(1, TOK), mask.reshape(1, TOK))
    return outs[0], outs[1].reshape(TOK), outs[2].reshape(TOK), outs[3].reshape(())


def solution(mesh):
    return jax.shard_map(
        on_device,
        mesh=mesh,
        in_specs=(P("dp", "vocab"), P("vocab", "dp", None), P("dp", "vocab"), P("dp"), P("dp")),
        out_specs=(P("dp", "vocab"), P("dp"), P("dp"), P()),
        check_vma=False,
    )
```

```python
import jax
import jax.numpy as jnp
from jax import lax
from jax.experimental import pallas as pl
from jax.experimental.pallas import tpu as pltpu
from jax.sharding import PartitionSpec as P

F32 = jnp.float32
BF16 = jnp.bfloat16
D = 2048
VT = 2432
TOK = 128
R = 64
NT = VT // 128
NZ = 16
MESH = pl.DeviceIdType.MESH

XP, YP, YM, ZP, CP = range(5)


def kernel(
    hid_hbm, blk_ref, tea_hbm, ids_hbm, mask_hbm,
    grad_ref, row_ref,
    w, ht, hg, acc, lt, tt, et, dl, stat, mrun, mgot, lrun, lgot, xsend, xrecv, own, zsend, zrecv,
    tea_ref, ids_ref, mask_ref,
    w_send, w_recv, d_send, d_recv, loc_sem, h_send, h_recv,
    s_send, s_recv, m_send, m_recv, l_send, l_recv, x_send, x_recv, z_send, z_recv, ready,
):
    d = lax.axis_index("dp")
    v = lax.axis_index("vocab")
    xl, y, c = d // 8, (d // 2) % 4, d % 2
    xh, z = v // NZ, v % NZ
    h = v % 2

    def dev(dp, vocab):
        return {"dp": dp, "vocab": vocab}

    def along_z(k):
        return dev(d, xh * NZ + (z + k) % NZ)

    target = {
        XP: dev(d ^ 8, v),
        YP: dev(xl * 8 + ((y + 1) % 4) * 2 + c, v),
        YM: dev(xl * 8 + ((y + 3) % 4) * 2 + c, v),
        ZP: dev(d, v ^ 1),
        CP: dev(d ^ 1, v),
    }
    across_x = dev(d, v ^ NZ)
    ladder = [target[CP], target[XP], dev(xl * 8 + (y ^ 1) * 2 + c, v), dev(xl * 8 + (3 - y) * 2 + c, v)]
    far = [8, 7, 9, 6, 10, 5, 11, 4, 12, 3, 13, 2, 14, 1, 15]
    mine = pl.ds(pl.multiple_of(xh * R, R), R)
    theirs = pl.ds(pl.multiple_of((1 - xh) * R, R), R)

    barrier = pltpu.get_barrier_semaphore()
    for to in (target[YP], target[YM], target[XP], target[CP], along_z(1), along_z(15), across_x):
        pl.semaphore_signal(barrier, inc=1, device_id=to, device_id_type=MESH)
    near = blk_ref.at[:, pl.ds(pl.multiple_of(h * VT, 128), VT)]
    away = blk_ref.at[:, pl.ds(pl.multiple_of((1 - h) * VT, 128), VT)]
    own_rows = pl.ds(pl.multiple_of(h * 1024 + R * d, R), R)
    fetches = [
        pltpu.make_async_copy(src, dst, loc_sem.at[i])
        for i, (src, dst) in enumerate(
            [
                (hid_hbm, ht.at[z, mine]),
                (mask_hbm, mask_ref),
                (tea_hbm, tea_ref),
                (ids_hbm, ids_ref),
                (near, w.at[own_rows]),
            ]
        )
    ]
    for fetch in fetches:
        fetch.start()
    fetches[0].wait()
    fetches[1].wait()
    mrun[0] = mask_ref[...].astype(F32)
    pl.semaphore_wait(barrier, 7)

    started = []

    def send(src, dst, ssem, rsem, to):
        copy = pltpu.make_async_remote_copy(
            src_ref=src, dst_ref=dst, send_sem=ssem, recv_sem=rsem, device_id=to, device_id_type=MESH
        )
        copy.start()
        started.append(copy)

    def arrived(dst, sem):
        pltpu.make_async_copy(dst, dst, sem).wait()

    def tell(i, *to):
        for device in to:
            pl.semaphore_signal(ready.at[i], inc=1, device_id=device, device_id_type=MESH)

    def climb(run, got, ssem, rsem, step):
        if step:
            arrived(got.at[step - 1], rsem.at[step - 1])
            run[step] = run[step - 1] + got[step - 1]
        if step < 4:
            send(run.at[step], got.at[step], ssem.at[step], rsem.at[step], ladder[step])

    def rows_of(u, dx, dy, core, sub=None):
        base = (h ^ (u // 2)) * 1024 + R * ((xl ^ dx) * 8 + ((y + dy) % 4) * 2 + core) + 32 * (u % 2)
        if sub is None:
            return pl.ds(pl.multiple_of(base, 32), 32)
        return pl.ds(pl.multiple_of(base + 16 * sub, 16), 16)

    counter = {"w": 0, "d": 0}
    subs = {(0, 1, 1, 0): 32, (0, 1, 3, 1): 33, (0, 1, 1, 1): None, (0, 1, 3, 0): None}

    def sem_of(u, dx, dy, sub=None):
        return subs.get((u, dx, dy, sub)) or u * 8 + dx * 4 + dy

    def pass_on(u, dx, dy, way, sub=None, src=None):
        ref = w.at[rows_of(u, dx, dy, c, sub)]
        if way == XP:
            at = (u, dx ^ 1, dy, sub)
        elif way == YP:
            at = (u, dx, (dy + 3) % 4, sub)
        elif way == YM:
            at = (u, dx, (dy + 1) % 4, sub)
        k = counter["w"]
        counter["w"] += 1
        send(ref if src is None else src, ref, w_send.at[k], w_recv.at[sem_of(*at)], target[way])

    def across(u, dx, dy):
        ref = w.at[rows_of(u, dx, dy, c)]
        k = counter["d"]
        counter["d"] += 1
        send(ref, ref, d_send.at[k], d_recv.at[sem_of(u, dx, dy)], target[CP])

    def piece_in(u, dx, dy, sub=None):
        arrived(w.at[rows_of(u, dx, dy, c, sub)], w_recv.at[sem_of(u, dx, dy, sub)])

    def peer_in(t, dx):
        for u in (2 * t, 2 * t + 1):
            for dy in range(4):
                if (u, dx, dy) != (1, 0, 0) and (u, dx, dy) != (0, 0, 0):
                    arrived(w.at[rows_of(u, dx, dy, 1 - c)], d_recv.at[sem_of(u, dx, dy)])

    for u in (0, 1):
        lines = pl.ds(32 * u, 32)
        for way in (XP, YP, YM):
            pass_on(u, 0, 0, way, src=near.at[lines])
        there = pl.ds(pl.multiple_of(h * 1024 + R * d + 32 * u, 32), 32)
        send(away.at[lines], w.at[there], w_send.at[46 + u], w_recv.at[sem_of(2 + u, 0, 0)], target[ZP])
    send(ht.at[z, mine], ht.at[z, mine], h_send.at[15], h_recv.at[1], across_x)
    send(near, w.at[own_rows], d_send.at[31], d_recv.at[0], target[CP])
    tell(0, along_z(1), along_z(15))
    climb(mrun, mgot, m_send, m_recv, 0)

    def turn_teacher(j, top):
        at = pl.ds(pl.multiple_of(j * 128, 128), 128)
        block = tea_ref[:, at].astype(F32).T
        tt[at, :] = block
        return jnp.maximum(top, block.reshape(16, 8, 128).max(axis=0))

    fetches[2].wait()
    top = lax.fori_loop(0, NT, turn_teacher, jnp.full((8, 128), -jnp.inf, F32))
    t_max = top.max(axis=0, keepdims=True)
    pl.semaphore_wait(ready.at[0], 2)
    tell(1, along_z(2), along_z(14))

    def exp_teacher(j, total):
        at = pl.ds(pl.multiple_of(j * 128, 128), 128)
        e = jnp.exp(tt[at, :] - t_max)
        et[at, :] = e
        return total + e.reshape(16, 8, 128).sum(axis=0)

    t_sum = lax.fori_loop(0, NT, exp_teacher, jnp.zeros((8, 128), F32)).sum(axis=0, keepdims=True)
    climb(mrun, mgot, m_send, m_recv, 1)

    hidden = iter(range(15))

    def spread(*steps):
        for k in steps:
            send(ht.at[z], ht.at[z], h_send.at[next(hidden)], h_recv.at[0], along_z(k))

    arrived(ht.at[z, theirs], h_recv.at[1])
    spread(1, 15, 2, 14)
    pl.semaphore_wait(ready.at[1], 2)
    tell(2, along_z(4), along_z(12))
    spread(3, 13, 4, 12)

    piece_in(0, 0, 3)
    pass_on(0, 0, 3, YP)
    across(0, 0, 3)
    piece_in(0, 0, 1)
    across(0, 0, 1)
    piece_in(2, 0, 0)
    pass_on(2, 0, 0, XP)
    pass_on(2, 0, 0, YP)
    pass_on(2, 0, 0, YM)
    pass_on(0, 0, 3, XP, sub=1)
    pass_on(0, 0, 1, XP, sub=0)
    across(2, 0, 0)
    piece_in(0, 1, 0)
    across(0, 1, 0)
    climb(mrun, mgot, m_send, m_recv, 2)
    piece_in(1, 0, 1)
    pass_on(1, 0, 1, YM)
    across(1, 0, 1)
    piece_in(1, 0, 3)
    across(1, 0, 3)
    piece_in(3, 0, 0)
    pass_on(3, 0, 0, YP)
    pass_on(3, 0, 0, YM)
    pass_on(3, 0, 0, XP)
    across(3, 0, 0)
    piece_in(1, 1, 0)
    across(1, 1, 0)
    pl.semaphore_wait(ready.at[2], 2)
    tell(3, across_x)
    spread(8, 7, 9, 6, 10, 5, 11)
    piece_in(0, 0, 2)
    pass_on(0, 0, 2, XP)
    across(0, 0, 2)
    piece_in(2, 0, 1)
    across(2, 0, 1)
    piece_in(2, 1, 0)
    across(2, 1, 0)
    climb(mrun, mgot, m_send, m_recv, 3)
    piece_in(2, 0, 3)
    pass_on(2, 0, 3, YP)
    across(2, 0, 3)
    piece_in(1, 0, 2)
    pass_on(1, 0, 2, XP)
    across(1, 0, 2)
    piece_in(3, 0, 1)
    pass_on(3, 0, 1, YM)
    across(3, 0, 1)
    for u in (0, 1, 2):
        pass_on(u, 1, 0, YP, sub=None if u else 0)
        pass_on(u, 1, 0, YM, sub=None if u else 1)
    piece_in(3, 0, 3)
    across(3, 0, 3)
    piece_in(3, 1, 0)
    pass_on(3, 1, 0, YP)
    pass_on(3, 1, 0, YM)
    across(3, 1, 0)
    piece_in(2, 0, 2)
    pass_on(2, 0, 2, XP)
    across(2, 0, 2)
    piece_in(3, 0, 2)
    pass_on(3, 0, 2, XP)
    across(3, 0, 2)
    piece_in(0, 1, 2)
    across(0, 1, 2)
    climb(mrun, mgot, m_send, m_recv, 4)

    arrived(ht.at[pl.ds(0, 15)], h_recv.at[0])
    for g in range(4):
        part = ht[8 * (g % 2) : 8 * (g % 2) + 8, (g // 2) * R : (g // 2) * R + R, :]
        hg[g] = part.reshape(512, TOK).astype(F32).T.astype(BF16)

    def multiply(t, dx, first):
        g = (h ^ t) * 2 + (xl ^ dx)
        rows = pl.ds(pl.multiple_of(g * 512, 512), 512)
        part = jnp.dot(hg[g], w[rows, :], preferred_element_type=F32)
        acc[...] = part if first else acc[...] + part

    fetches[4].wait()
    other_rows = pl.ds(pl.multiple_of(h * 1024 + R * (d ^ 1), R), R)
    arrived(w.at[other_rows], d_recv.at[0])
    peer_in(0, 0)
    multiply(0, 0, True)
    for dy in (3, 1):
        for sub in (0, 1):
            piece_in(0, 1, dy, sub)
        across(0, 1, dy)
    for dy in (2, 3, 1):
        piece_in(1, 1, dy)
        across(1, 1, dy)
    peer_in(1, 0)
    multiply(1, 0, False)
    for u in (2, 3):
        for dy in (2, 3, 1):
            piece_in(u, 1, dy)
            across(u, 1, dy)
        if u == 2:
            peer_in(0, 1)
            multiply(0, 1, False)
    peer_in(1, 1)
    multiply(1, 1, False)
    pl.semaphore_wait(ready.at[3], 1)
    fetches[3].wait()

    ids = ids_ref[...]

    def turn_student(j, carry):
        top, hit = carry
        at = pl.ds(pl.multiple_of(j * 128, 128), 128)
        block = acc[:, at].T
        lt[at, :] = block
        column = lax.broadcasted_iota(jnp.int32, (128, 128), 0) + (v * VT + j * 128)
        found = jnp.where(column == ids, block, 0.0)
        return (
            jnp.maximum(top, block.reshape(16, 8, 128).max(axis=0)),
            hit + found.reshape(16, 8, 128).sum(axis=0),
        )

    zero8 = jnp.zeros((8, 128), F32)
    top, hit = lax.fori_loop(0, NT, turn_student, (jnp.full((8, 128), -jnp.inf, F32), zero8))
    s_max = top.max(axis=0, keepdims=True)

    def exp_student(j, carry):
        total, cross = carry
        at = pl.ds(pl.multiple_of(j * 128, 128), 128)
        s = lt[at, :]
        e = jnp.exp(s - s_max)
        x = et[at, :] * (tt[at, :] - s)
        lt[at, :] = e
        return total + e.reshape(16, 8, 128).sum(axis=0), cross + x.reshape(16, 8, 128).sum(axis=0)

    total, cross = lax.fori_loop(0, NT, exp_student, (zero8, zero8))
    s_sum = total.sum(axis=0, keepdims=True)
    x_sum = cross.sum(axis=0, keepdims=True)
    s_hit = hit.sum(axis=0, keepdims=True)
    stat[v] = jnp.concatenate([t_max, s_max, t_sum, x_sum, s_sum, s_hit, s_hit, s_hit], axis=0)

    k = 0
    for offset in far + [0]:
        for other in (1, 0):
            if other or offset:
                to = dev(d, (xh ^ other) * NZ + (z + offset) % NZ)
                send(stat.at[v], stat.at[v], s_send.at[k], s_recv, to)
                k += 1
    count = jnp.sum(mrun[4], axis=1, keepdims=True)
    factor = mask_ref[...].astype(F32) / count
    arrived(stat.at[pl.ds(0, 31)], s_recv)
    tops = stat[0]
    for r in range(1, 32):
        tops = jnp.maximum(tops, stat[r])
    tops = tops[0:2]
    tz = xz = sz = hz = jnp.zeros((1, 128), F32)
    for r in range(32):
        one = stat[r]
        scale = jnp.exp(one[0:2] - tops)
        tz = tz + scale[0:1] * one[2:3]
        xz = xz + scale[0:1] * one[3:4]
        sz = sz + scale[1:2] * one[4:5]
        hz = hz + one[5:6]
    t_lse = tops[0:1] + jnp.log(tz)
    s_lse = tops[1:2] + jnp.log(sz)
    kl = xz / tz - t_lse + s_lse
    row_ref[0:1] = kl
    row_ref[1:2] = hz - s_lse
    lrun[0] = kl * mask_ref[...].astype(F32)
    climb(lrun, lgot, l_send, l_recv, 0)

    s_scale = factor * (jnp.exp(s_max - tops[1:2]) / sz)
    t_scale = factor * (jnp.exp(t_max - tops[0:1]) / tz)

    def make_dl(j, _):
        at = pl.ds(pl.multiple_of(j * 128, 128), 128)
        dl[at, :] = (lt[at, :] * s_scale - et[at, :] * t_scale).astype(BF16)
        return 0

    lax.fori_loop(0, NT, make_dl, 0)

    def quarter(half, q):
        rows = pl.ds(pl.multiple_of(half * 1024 + q * 256, 256), 256)
        return jnp.dot(w[rows, :], dl[...], preferred_element_type=F32)

    order = (0, 1, 3, 2)
    for step, q in enumerate(order):
        xsend[q] = quarter(1 - xh, q).astype(BF16)
        send(xsend.at[q], xrecv.at[q], x_send.at[q], x_recv.at[q], across_x)
    climb(lrun, lgot, l_send, l_recv, 1)
    for q in order:
        own[q] = quarter(xh, q)
    climb(lrun, lgot, l_send, l_recv, 2)
    elsewhere = []
    for q in order:
        arrived(xrecv.at[q], x_recv.at[q])
        both = own[q] + xrecv[q].astype(F32)
        own[q] = both
        zsend[q] = both.astype(BF16)
        for r in range(4):
            zt = q * 4 + r
            copy = pltpu.make_async_remote_copy(
                src_ref=zsend.at[q, pl.ds(r * R, R)],
                dst_ref=zrecv.at[z],
                send_sem=z_send.at[zt],
                recv_sem=z_recv,
                device_id=dev(d, xh * NZ + zt),
                device_id_type=MESH,
            )
            pl.when(z != zt)(copy.start)
            elsewhere.append((zt, copy))

    climb(lrun, lgot, l_send, l_recv, 3)
    climb(lrun, lgot, l_send, l_recv, 4)
    loss = jnp.sum(lrun[4], axis=1, keepdims=True) / count
    row_ref[2:3] = jnp.broadcast_to(loss, (1, TOK))

    kept = own[z // 4, pl.ds(pl.multiple_of((z % 4) * R, R), R), :]
    arrived(zrecv.at[pl.ds(0, 15)], z_recv)
    for r in range(1, 16):
        kept = kept + zrecv[z ^ r].astype(F32)
    grad_ref[...] = kept.astype(BF16)
    for zt, copy in elsewhere:
        pl.when(z != zt)(copy.wait_send)
    for copy in started:
        copy.wait_send()


def place(grad_in, row_in, grad_ref, kl_ref, samp_ref, loss_ref):
    grad_ref[...] = grad_in[...]
    kl_ref[...] = row_in[0]
    samp_ref[...] = row_in[1]
    loss_ref[...] = row_in[2:3, 0:1]


def on_device(hidden, blocks, teacher, ids, mask):
    vm = pl.BlockSpec(memory_space=pltpu.VMEM)
    hbm = pl.BlockSpec(memory_space=pl.ANY)
    dma = pltpu.SemaphoreType.DMA
    grad, rows = pl.pallas_call(
        kernel,
        out_shape=(jax.ShapeDtypeStruct((R, TOK), BF16), jax.ShapeDtypeStruct((8, TOK), F32)),
        in_specs=[hbm] * 5,
        out_specs=(vm, vm),
        scratch_shapes=[
            pltpu.VMEM((D, VT), BF16),
            pltpu.VMEM((NZ, 2 * R, TOK), BF16),
            pltpu.VMEM((4, TOK, 512), BF16),
            pltpu.VMEM((TOK, VT), F32),
            pltpu.VMEM((VT, TOK), F32),
            pltpu.VMEM((VT, TOK), F32),
            pltpu.VMEM((VT, TOK), F32),
            pltpu.VMEM((VT, TOK), BF16),
            pltpu.VMEM((32, 8, TOK), F32),
            pltpu.VMEM((5, 1, TOK), F32),
            pltpu.VMEM((4, 1, TOK), F32),
            pltpu.VMEM((5, 1, TOK), F32),
            pltpu.VMEM((4, 1, TOK), F32),
            pltpu.VMEM((4, 256, TOK), BF16),
            pltpu.VMEM((4, 256, TOK), BF16),
            pltpu.VMEM((4, 256, TOK), F32),
            pltpu.VMEM((4, 256, TOK), BF16),
            pltpu.VMEM((NZ, R, TOK), BF16),
            pltpu.VMEM((TOK, VT), BF16),
            pltpu.VMEM((1, TOK), jnp.int32),
            pltpu.VMEM((1, TOK), jnp.int32),
            dma((48,)), dma((34,)), dma((32,)), dma((32,)), dma((5,)), dma((16,)), dma((2,)),
            dma((31,)), dma, dma((4,)), dma((4,)), dma((4,)), dma((4,)), dma((4,)), dma((4,)), dma((16,)), dma,
            pltpu.SemaphoreType.REGULAR((4,)),
        ],
        compiler_params=pltpu.CompilerParams(
            collective_id=0, has_side_effects=True, vmem_limit_bytes=60 * 1024 * 1024
        ),
    )(hidden.T, blocks.reshape(R, 2 * VT), teacher, ids.reshape(1, TOK), mask.reshape(1, TOK))
    grad, kl, samp, loss = pl.pallas_call(
        place,
        out_shape=(
            jax.ShapeDtypeStruct((R, TOK), BF16),
            jax.ShapeDtypeStruct((TOK,), F32),
            jax.ShapeDtypeStruct((TOK,), F32),
            jax.ShapeDtypeStruct((1, 1), F32),
        ),
        in_specs=[vm, vm],
        out_specs=(vm, vm, vm, vm),
    )(grad, rows)
    return grad.T, kl, samp, loss.reshape(())


def solution(mesh):
    return jax.shard_map(
        on_device,
        mesh=mesh,
        in_specs=(P("dp", "vocab"), P("vocab", "dp", None), P("dp", "vocab"), P("dp"), P("dp")),
        out_specs=(P("dp", "vocab"), P("dp"), P("dp"), P()),
        check_vma=False,
    )
```

```python
import jax
import jax.numpy as jnp
from jax import lax
from jax.experimental import pallas as pl
from jax.experimental.pallas import tpu as pltpu
from jax.sharding import PartitionSpec as P

F32 = jnp.float32
BF16 = jnp.bfloat16
D = 2048
VT = 2432
TOK = 128
R = 64
NT = VT // 128
CUT = 1280
COLS = (pl.ds(0, CUT), pl.ds(CUT, VT - CUT))
TILES = (range(CUT // 128), range(CUT // 128, NT))
NZ = 16
MESH = pl.DeviceIdType.MESH

XP, YP, YM, ZP, CP = range(5)


def kernel(
    hid_hbm, blk_ref, tea_hbm, ids_hbm, mask_hbm,
    grad_ref, row_ref,
    w, ht, hg, acc, lt, tt, et, dl, stat, mrun, mgot, lrun, lgot, xsend, xrecv, own, zsend, zrecv,
    tea_ref, ids_ref, mask_ref,
    w_send, w_recv, d_send, d_recv, loc_sem, h_send, h_recv,
    s_send, s_recv, m_send, m_recv, l_send, l_recv, x_send, x_recv, z_send, z_recv, ready,
):
    d = lax.axis_index("dp")
    v = lax.axis_index("vocab")
    xl, y, c = d // 8, (d // 2) % 4, d % 2
    xh, z = v // NZ, v % NZ
    h = v % 2

    def dev(dp, vocab):
        return {"dp": dp, "vocab": vocab}

    def along_z(k):
        return dev(d, xh * NZ + (z + k) % NZ)

    target = {
        XP: dev(d ^ 8, v),
        YP: dev(xl * 8 + ((y + 1) % 4) * 2 + c, v),
        YM: dev(xl * 8 + ((y + 3) % 4) * 2 + c, v),
        ZP: dev(d, v ^ 1),
        CP: dev(d ^ 1, v),
    }
    across_x = dev(d, v ^ NZ)
    ladder = [target[CP], target[XP], dev(xl * 8 + (y ^ 1) * 2 + c, v), dev(xl * 8 + (3 - y) * 2 + c, v)]
    far = [8, 7, 9, 6, 10, 5, 11, 4, 12, 3, 13, 2, 14, 1, 15]
    mine = pl.ds(pl.multiple_of(xh * R, R), R)
    theirs = pl.ds(pl.multiple_of((1 - xh) * R, R), R)

    barrier = pltpu.get_barrier_semaphore()
    for to in (target[YP], target[YM], target[XP], target[CP], along_z(1), along_z(15), across_x):
        pl.semaphore_signal(barrier, inc=1, device_id=to, device_id_type=MESH)
    near = blk_ref.at[:, pl.ds(pl.multiple_of(h * VT, 128), VT)]
    away = blk_ref.at[:, pl.ds(pl.multiple_of((1 - h) * VT, 128), VT)]
    own_rows = pl.ds(pl.multiple_of(h * 1024 + R * d, R), R)
    fetches = [
        pltpu.make_async_copy(src, dst, loc_sem.at[i])
        for i, (src, dst) in enumerate(
            [
                (hid_hbm, ht.at[z, mine]),
                (mask_hbm, mask_ref),
                (tea_hbm, tea_ref),
                (ids_hbm, ids_ref),
                (near, w.at[own_rows]),
            ]
        )
    ]
    for fetch in fetches:
        fetch.start()
    fetches[0].wait()
    fetches[1].wait()
    mrun[0] = mask_ref[...].astype(F32)
    pl.semaphore_wait(barrier, 7)

    started = []

    def send(src, dst, ssem, rsem, to):
        copy = pltpu.make_async_remote_copy(
            src_ref=src, dst_ref=dst, send_sem=ssem, recv_sem=rsem, device_id=to, device_id_type=MESH
        )
        copy.start()
        started.append(copy)

    def arrived(dst, sem):
        pltpu.make_async_copy(dst, dst, sem).wait()

    def tell(i, *to):
        for device in to:
            pl.semaphore_signal(ready.at[i], inc=1, device_id=device, device_id_type=MESH)

    def climb(run, got, ssem, rsem, step):
        if step:
            arrived(got.at[step - 1], rsem.at[step - 1])
            run[step] = run[step - 1] + got[step - 1]
        if step < 4:
            send(run.at[step], got.at[step], ssem.at[step], rsem.at[step], ladder[step])

    def unit(u, dx, dy, core, sub=None):
        base = (h ^ (u // 2)) * 1024 + R * ((xl ^ dx) * 8 + ((y + dy) % 4) * 2 + core)
        if sub is None:
            return w.at[pl.ds(pl.multiple_of(base, R), R), COLS[u % 2]]
        return w.at[pl.ds(pl.multiple_of(base + 32 * sub, 32), 32), COLS[u % 2]]

    counter = {"w": 0, "d": 0}
    subs = {(0, 1, 1, 0): 32, (0, 1, 3, 1): 33, (0, 1, 1, 1): None, (0, 1, 3, 0): None}

    def sem_of(u, dx, dy, sub=None):
        return subs.get((u, dx, dy, sub)) or u * 8 + dx * 4 + dy

    def pass_on(u, dx, dy, way, sub=None, src=None):
        ref = unit(u, dx, dy, c, sub)
        if way == XP:
            at = (u, dx ^ 1, dy, sub)
        elif way == YP:
            at = (u, dx, (dy + 3) % 4, sub)
        elif way == YM:
            at = (u, dx, (dy + 1) % 4, sub)
        k = counter["w"]
        counter["w"] += 1
        send(ref if src is None else src, ref, w_send.at[k], w_recv.at[sem_of(*at)], target[way])

    def across(u, dx, dy):
        ref = unit(u, dx, dy, c)
        k = counter["d"]
        counter["d"] += 1
        send(ref, ref, d_send.at[k], d_recv.at[sem_of(u, dx, dy)], target[CP])

    def piece_in(u, dx, dy, sub=None):
        arrived(unit(u, dx, dy, c, sub), w_recv.at[sem_of(u, dx, dy, sub)])

    def peer_in(u, dx):
        for dy in range(4):
            if (u, dx, dy) not in ((0, 0, 0), (1, 0, 0)):
                arrived(unit(u, dx, dy, 1 - c), d_recv.at[sem_of(u, dx, dy)])

    for u in (0, 1):
        for way in (XP, YP, YM):
            pass_on(u, 0, 0, way, src=near.at[:, COLS[u]])
        send(away.at[:, COLS[u]], w.at[own_rows, COLS[u]], w_send.at[46 + u], w_recv.at[sem_of(2 + u, 0, 0)], target[ZP])
    send(ht.at[z, mine], ht.at[z, mine], h_send.at[15], h_recv.at[1], across_x)
    send(near, w.at[own_rows], d_send.at[31], d_recv.at[0], target[CP])
    tell(0, along_z(1), along_z(15))
    climb(mrun, mgot, m_send, m_recv, 0)

    fetches[2].wait()
    def fold(block, how):
        return how(block.reshape(16, 8, 128), axis=0)

    def tile(j):
        return slice(j * 128, j * 128 + 128)

    low8 = jnp.full((8, 128), -jnp.inf, F32)
    zero8 = jnp.zeros((8, 128), F32)
    top = low8
    for j in range(NT):
        block = tea_ref[:, tile(j)].astype(F32).T
        tt[tile(j), :] = block
        top = jnp.maximum(top, fold(block, jnp.max))
    t_max = top.max(axis=0, keepdims=True)
    pl.semaphore_wait(ready.at[0], 2)
    tell(1, along_z(2), along_z(14))

    total = zero8
    for j in range(NT):
        e = jnp.exp(tt[tile(j), :] - t_max)
        et[tile(j), :] = e
        total = total + fold(e, jnp.sum)
    t_sum = total.sum(axis=0, keepdims=True)
    climb(mrun, mgot, m_send, m_recv, 1)

    hidden = iter(range(15))

    def spread(source, *steps):
        for k in steps:
            rsem = {4: 2, 12: 3}.get(k, 0) if source is z else 0
            send(ht.at[source], ht.at[source], h_send.at[next(hidden)], h_recv.at[rsem], along_z(k))

    arrived(ht.at[z, theirs], h_recv.at[1])
    spread(z, 1, 15, 2, 14)
    pl.semaphore_wait(ready.at[1], 2)
    tell(2, along_z(4), along_z(12))
    spread(z, 3, 13, 4, 12)

    piece_in(0, 0, 3)
    pass_on(0, 0, 3, YP)
    across(0, 0, 3)
    piece_in(0, 0, 1)
    across(0, 0, 1)
    piece_in(2, 0, 0)
    pass_on(2, 0, 0, XP)
    pass_on(2, 0, 0, YP)
    pass_on(2, 0, 0, YM)
    pass_on(0, 0, 3, XP, sub=1)
    pass_on(0, 0, 1, XP, sub=0)
    across(2, 0, 0)
    piece_in(0, 1, 0)
    across(0, 1, 0)
    climb(mrun, mgot, m_send, m_recv, 2)
    piece_in(1, 0, 1)
    pass_on(1, 0, 1, YM)
    across(1, 0, 1)
    piece_in(1, 0, 3)
    across(1, 0, 3)
    piece_in(3, 0, 0)
    pass_on(3, 0, 0, YP)
    pass_on(3, 0, 0, YM)
    pass_on(3, 0, 0, XP)
    across(3, 0, 0)
    piece_in(1, 1, 0)
    across(1, 1, 0)
    piece_in(0, 0, 2)
    pass_on(0, 0, 2, XP)
    across(0, 0, 2)
    piece_in(2, 0, 1)
    across(2, 0, 1)
    piece_in(2, 1, 0)
    across(2, 1, 0)
    climb(mrun, mgot, m_send, m_recv, 3)
    piece_in(2, 0, 3)
    pass_on(2, 0, 3, YP)
    across(2, 0, 3)
    piece_in(1, 0, 2)
    pass_on(1, 0, 2, XP)
    across(1, 0, 2)
    before, after = (z + 12) % NZ, (z + 4) % NZ
    arrived(ht.at[before], h_recv.at[2])
    spread(before, 4, 3, 2, 1)
    arrived(ht.at[after], h_recv.at[3])
    spread(after, 13, 14, 15)
    piece_in(3, 0, 1)
    pass_on(3, 0, 1, YM)
    across(3, 0, 1)
    for u in (0, 1, 2):
        pass_on(u, 1, 0, YP, sub=None if u else 0)
        pass_on(u, 1, 0, YM, sub=None if u else 1)
    piece_in(3, 0, 3)
    across(3, 0, 3)
    piece_in(3, 1, 0)
    pass_on(3, 1, 0, YP)
    pass_on(3, 1, 0, YM)
    across(3, 1, 0)
    piece_in(2, 0, 2)
    pass_on(2, 0, 2, XP)
    across(2, 0, 2)
    piece_in(3, 0, 2)
    pass_on(3, 0, 2, XP)
    across(3, 0, 2)
    piece_in(0, 1, 2)
    across(0, 1, 2)
    climb(mrun, mgot, m_send, m_recv, 4)

    pl.semaphore_wait(ready.at[2], 2)
    tell(3, across_x)

    arrived(ht.at[pl.ds(0, 13)], h_recv.at[0])
    for g in range(4):
        part = ht[8 * (g % 2) : 8 * (g % 2) + 8, (g // 2) * R : (g // 2) * R + R, :]
        hg[g] = part.reshape(512, TOK).astype(F32).T.astype(BF16)

    def multiply(u, dx):
        g = (h ^ (u // 2)) * 2 + (xl ^ dx)
        rows = pl.ds(pl.multiple_of(g * 512, 512), 512)
        cols = COLS[u % 2]
        part = jnp.dot(hg[g], w[rows, cols], preferred_element_type=F32)
        acc[:, cols] = part if (u // 2, dx) == (0, 0) else acc[:, cols] + part

    def statistics(p):
        top, hit = low8, zero8
        for j in TILES[p]:
            block = acc[:, tile(j)].T
            lt[tile(j), :] = block
            column = lax.broadcasted_iota(jnp.int32, (128, 128), 0) + (v * VT + j * 128)
            top = jnp.maximum(top, fold(block, jnp.max))
            hit = hit + fold(jnp.where(column == ids, block, 0.0), jnp.sum)
        high = top.max(axis=0, keepdims=True)
        total, cross = zero8, zero8
        for j in TILES[p]:
            logit = lt[tile(j), :]
            e = jnp.exp(logit - high)
            lt[tile(j), :] = e
            total = total + fold(e, jnp.sum)
            cross = cross + fold(et[tile(j), :] * (tt[tile(j), :] - logit), jnp.sum)
        return high, *(a.sum(axis=0, keepdims=True) for a in (total, cross, hit))

    fetches[3].wait()
    ids = ids_ref[...]
    fetches[4].wait()
    other_rows = pl.ds(pl.multiple_of(h * 1024 + R * (d ^ 1), R), R)
    arrived(w.at[other_rows], d_recv.at[0])
    for u in (0, 1):
        peer_in(u, 0)
        multiply(u, 0)
    for dy in (3, 1):
        for sub in (0, 1):
            piece_in(0, 1, dy, sub)
        across(0, 1, dy)
    for u in (2, 3):
        peer_in(u, 0)
        multiply(u, 0)
    for dy in (2, 3, 1):
        piece_in(1, 1, dy)
        across(1, 1, dy)
    peer_in(0, 1)
    multiply(0, 1)
    for dy in (2, 3, 1):
        piece_in(2, 1, dy)
        across(2, 1, dy)
    peer_in(1, 1)
    multiply(1, 1)
    peer_in(2, 1)
    multiply(2, 1)
    piece_in(3, 1, 2)
    across(3, 1, 2)
    max_0, sum_0, cross_0, hit_0 = statistics(0)
    for dy in (3, 1):
        piece_in(3, 1, dy)
        across(3, 1, dy)
    pl.semaphore_wait(ready.at[3], 1)
    peer_in(3, 1)
    multiply(3, 1)
    max_1, sum_1, cross_1, hit_1 = statistics(1)
    s_max = jnp.maximum(max_0, max_1)
    s_sum = sum_0 * jnp.exp(max_0 - s_max) + sum_1 * jnp.exp(max_1 - s_max)
    x_sum = cross_0 + cross_1
    s_hit = hit_0 + hit_1
    stat[v] = jnp.concatenate([t_max, s_max, t_sum, x_sum, s_sum, s_hit, s_hit, s_hit], axis=0)

    k = 0
    for offset in far + [0]:
        for other in (1, 0):
            if other or offset:
                to = dev(d, (xh ^ other) * NZ + (z + offset) % NZ)
                send(stat.at[v], stat.at[v], s_send.at[k], s_recv, to)
                k += 1
    count = jnp.sum(mrun[4], axis=1, keepdims=True)
    factor = mask_ref[...].astype(F32) / count
    arrived(stat.at[pl.ds(0, 31)], s_recv)
    tops = stat[0]
    for r in range(1, 32):
        tops = jnp.maximum(tops, stat[r])
    tops = tops[0:2]
    tz = xz = sz = hz = jnp.zeros((1, 128), F32)
    for r in range(32):
        one = stat[r]
        scale = jnp.exp(one[0:2] - tops)
        tz = tz + scale[0:1] * one[2:3]
        xz = xz + scale[0:1] * one[3:4]
        sz = sz + scale[1:2] * one[4:5]
        hz = hz + one[5:6]
    t_lse = tops[0:1] + jnp.log(tz)
    s_lse = tops[1:2] + jnp.log(sz)
    kl = xz / tz - t_lse + s_lse
    row_ref[0:1] = kl
    row_ref[1:2] = hz - s_lse
    lrun[0] = kl * mask_ref[...].astype(F32)
    climb(lrun, lgot, l_send, l_recv, 0)

    t_scale = factor * (jnp.exp(t_max - tops[0:1]) / tz)
    for p, high in enumerate((max_0, max_1)):
        s_scale = factor * (jnp.exp(high - tops[1:2]) / sz)
        for j in TILES[p]:
            dl[tile(j), :] = (lt[tile(j), :] * s_scale - et[tile(j), :] * t_scale).astype(BF16)

    def quarter(half, q):
        rows = pl.ds(pl.multiple_of(half * 1024 + q * 256, 256), 256)
        return jnp.dot(w[rows, :], dl[...], preferred_element_type=F32)

    zq = z // 4
    first, second = 2 * ((3 - zq) // 3), 3 - 2 * (zq // 2)
    order = (first, second, 6 - first - second - zq, zq)
    for i, q in enumerate(order):
        xsend[i] = quarter(1 - xh, q).astype(BF16)
        send(xsend.at[i], xrecv.at[i], x_send.at[i], x_recv.at[i], across_x)
    climb(lrun, lgot, l_send, l_recv, 1)
    for i, q in enumerate(order):
        own[i] = quarter(xh, q)
    climb(lrun, lgot, l_send, l_recv, 2)
    k = 0
    for i, q in enumerate(order):
        arrived(xrecv.at[i], x_recv.at[i])
        both = own[i] + xrecv[i].astype(F32)
        own[i] = both
        zsend[i] = both.astype(BF16)
        for r in range(4) if i < 3 else (2, 3, 1):
            zt = q * 4 + r if i < 3 else z ^ r
            piece = zsend.at[i, pl.ds(pl.multiple_of((zt % 4) * R, R), R)]
            send(piece, zrecv.at[z], z_send.at[k], z_recv, dev(d, xh * NZ + zt))
            k += 1

    climb(lrun, lgot, l_send, l_recv, 3)
    climb(lrun, lgot, l_send, l_recv, 4)
    loss = jnp.sum(lrun[4], axis=1, keepdims=True) / count
    row_ref[2:3] = jnp.broadcast_to(loss, (1, TOK))

    kept = own[3, pl.ds(pl.multiple_of((z % 4) * R, R), R), :]
    arrived(zrecv.at[pl.ds(0, 15)], z_recv)
    for r in range(1, 16):
        kept = kept + zrecv[z ^ r].astype(F32)
    grad_ref[...] = kept.astype(BF16)
    for copy in started:
        copy.wait_send()


def place(grad_in, row_in, grad_ref, kl_ref, samp_ref, loss_ref):
    grad_ref[...] = grad_in[...]
    kl_ref[...] = row_in[0]
    samp_ref[...] = row_in[1]
    loss_ref[...] = row_in[2:3, 0:1]


def on_device(hidden, blocks, teacher, ids, mask):
    vm = pl.BlockSpec(memory_space=pltpu.VMEM)
    hbm = pl.BlockSpec(memory_space=pl.ANY)
    dma = pltpu.SemaphoreType.DMA
    grad, rows = pl.pallas_call(
        kernel,
        out_shape=(jax.ShapeDtypeStruct((R, TOK), BF16), jax.ShapeDtypeStruct((8, TOK), F32)),
        in_specs=[hbm] * 5,
        out_specs=(vm, vm),
        scratch_shapes=[
            pltpu.VMEM((D, VT), BF16),
            pltpu.VMEM((NZ, 2 * R, TOK), BF16),
            pltpu.VMEM((4, TOK, 512), BF16),
            pltpu.VMEM((TOK, VT), F32),
            pltpu.VMEM((VT, TOK), F32),
            pltpu.VMEM((VT, TOK), F32),
            pltpu.VMEM((VT, TOK), F32),
            pltpu.VMEM((VT, TOK), BF16),
            pltpu.VMEM((32, 8, TOK), F32),
            pltpu.VMEM((5, 1, TOK), F32),
            pltpu.VMEM((4, 1, TOK), F32),
            pltpu.VMEM((5, 1, TOK), F32),
            pltpu.VMEM((4, 1, TOK), F32),
            pltpu.VMEM((4, 256, TOK), BF16),
            pltpu.VMEM((4, 256, TOK), BF16),
            pltpu.VMEM((4, 256, TOK), F32),
            pltpu.VMEM((4, 256, TOK), BF16),
            pltpu.VMEM((NZ, R, TOK), BF16),
            pltpu.VMEM((TOK, VT), BF16),
            pltpu.VMEM((1, TOK), jnp.int32),
            pltpu.VMEM((1, TOK), jnp.int32),
            dma((48,)), dma((34,)), dma((32,)), dma((32,)), dma((5,)), dma((16,)), dma((4,)),
            dma((31,)), dma, dma((4,)), dma((4,)), dma((4,)), dma((4,)), dma((4,)), dma((4,)), dma((16,)), dma,
            pltpu.SemaphoreType.REGULAR((4,)),
        ],
        compiler_params=pltpu.CompilerParams(
            collective_id=0, has_side_effects=True, vmem_limit_bytes=60 * 1024 * 1024
        ),
    )(hidden.T, blocks.reshape(R, 2 * VT), teacher, ids.reshape(1, TOK), mask.reshape(1, TOK))
    grad, kl, samp, loss = pl.pallas_call(
        place,
        out_shape=(
            jax.ShapeDtypeStruct((R, TOK), BF16),
            jax.ShapeDtypeStruct((TOK,), F32),
            jax.ShapeDtypeStruct((TOK,), F32),
            jax.ShapeDtypeStruct((1, 1), F32),
        ),
        in_specs=[vm, vm],
        out_specs=(vm, vm, vm, vm),
    )(grad, rows)
    return grad.T, kl, samp, loss.reshape(())


def solution(mesh):
    return jax.shard_map(
        on_device,
        mesh=mesh,
        in_specs=(P("dp", "vocab"), P("vocab", "dp", None), P("dp", "vocab"), P("dp"), P("dp")),
        out_specs=(P("dp", "vocab"), P("dp"), P("dp"), P()),
        check_vma=False,
    )
```

```python
import jax
import jax.numpy as jnp
from jax import lax
from jax.experimental import pallas as pl
from jax.experimental.pallas import tpu as pltpu
from jax.sharding import PartitionSpec as P

F32 = jnp.float32
BF16 = jnp.bfloat16
D = 2048
VT = 2432
TOK = 128
R = 64
NT = VT // 128
CUTS = (0, 1280, 2048, VT)
COLS = tuple(pl.ds(a, b - a) for a, b in zip(CUTS, CUTS[1:]))
TILES = tuple(range(a // 128, b // 128) for a, b in zip(CUTS, CUTS[1:]))
NZ = 16
MESH = pl.DeviceIdType.MESH

XP, YP, YM, ZP, CP = range(5)


def kernel(
    hid_hbm, blk_ref, tea_hbm, ids_hbm, mask_hbm,
    grad_ref, row_ref,
    w, ht, hg, acc, lt, tt, et, dl, stat, tstat, away, mrun, mgot, lrun, lgot, xsend, xrecv, own, zsend, zrecv,
    tea_ref, ids_ref, mask_ref,
    w_send, w_recv, d_send, d_recv, loc_sem, h_send, h_recv,
    s_send, s_recv, t_send, t_recv, m_send, m_recv, l_send, l_recv, x_send, x_recv, z_send, z_recv, ready,
):
    d = lax.axis_index("dp")
    v = lax.axis_index("vocab")
    xl, y, c = d // 8, (d // 2) % 4, d % 2
    xh, z = v // NZ, v % NZ
    h = v % 2

    def dev(dp, vocab):
        return {"dp": dp, "vocab": vocab}

    def along_z(k):
        return dev(d, xh * NZ + (z + k) % NZ)

    target = {
        XP: dev(d ^ 8, v),
        YP: dev(xl * 8 + ((y + 1) % 4) * 2 + c, v),
        YM: dev(xl * 8 + ((y + 3) % 4) * 2 + c, v),
        ZP: dev(d, v ^ 1),
        CP: dev(d ^ 1, v),
    }
    across_x = dev(d, v ^ NZ)
    ladder = [target[CP], target[XP], dev(xl * 8 + (y ^ 1) * 2 + c, v), dev(xl * 8 + (3 - y) * 2 + c, v)]
    far = [8, 7, 9, 6, 10, 5, 11, 4, 12, 3, 13, 2, 14, 1, 15]
    mine = pl.ds(pl.multiple_of(xh * R, R), R)
    theirs = pl.ds(pl.multiple_of((1 - xh) * R, R), R)

    barrier = pltpu.get_barrier_semaphore()
    for to in (target[YP], target[YM], target[XP], target[CP], along_z(1), along_z(15), across_x):
        pl.semaphore_signal(barrier, inc=1, device_id=to, device_id_type=MESH)
    near = blk_ref.at[:, pl.ds(pl.multiple_of(h * VT, 128), VT)]
    rest = blk_ref.at[:, pl.ds(pl.multiple_of((1 - h) * VT, 128), VT)]
    own_rows = pl.ds(pl.multiple_of(h * 1024 + R * d, R), R)
    fetches = [
        pltpu.make_async_copy(src, dst, loc_sem.at[i])
        for i, (src, dst) in enumerate(
            [
                (near, w.at[own_rows]),
                (rest, away),
                (hid_hbm, ht.at[z, mine]),
                (mask_hbm, mask_ref),
                (tea_hbm, tea_ref),
                (ids_hbm, ids_ref),
            ]
        )
    ]
    for fetch in fetches:
        fetch.start()
    fetches[3].wait()
    mrun[0] = mask_ref[...].astype(F32)
    for fetch in fetches[:3]:
        fetch.wait()
    pl.semaphore_wait(barrier, 7)

    started = []

    def send(src, dst, ssem, rsem, to):
        copy = pltpu.make_async_remote_copy(
            src_ref=src, dst_ref=dst, send_sem=ssem, recv_sem=rsem, device_id=to, device_id_type=MESH
        )
        copy.start()
        started.append(copy)

    def arrived(dst, sem):
        pltpu.make_async_copy(dst, dst, sem).wait()

    def tell(i, *to):
        for device in to:
            pl.semaphore_signal(ready.at[i], inc=1, device_id=device, device_id_type=MESH)

    def climb(run, got, ssem, rsem, step):
        if step:
            arrived(got.at[step - 1], rsem.at[step - 1])
            run[step] = run[step - 1] + got[step - 1]
        if step < 4:
            send(run.at[step], got.at[step], ssem.at[step], rsem.at[step], ladder[step])

    def unit(u, dx, dy, core, sub=None):
        base = (h ^ (u // 3)) * 1024 + R * ((xl ^ dx) * 8 + ((y + dy) % 4) * 2 + core)
        if sub is None:
            return w.at[pl.ds(pl.multiple_of(base, R), R), COLS[u % 3]]
        return w.at[pl.ds(pl.multiple_of(base + 32 * sub, 32), 32), COLS[u % 3]]

    counter = {"w": 0, "d": 0}
    subs = {(0, 1, 1, 0): 48, (0, 1, 3, 1): 49, (0, 1, 1, 1): None, (0, 1, 3, 0): None}

    def sem_of(u, dx, dy, sub=None):
        return subs.get((u, dx, dy, sub)) or u * 8 + dx * 4 + dy

    def pass_on(u, dx, dy, way, sub=None):
        ref = unit(u, dx, dy, c, sub)
        if way == XP:
            at = (u, dx ^ 1, dy, sub)
        elif way == YP:
            at = (u, dx, (dy + 3) % 4, sub)
        elif way == YM:
            at = (u, dx, (dy + 1) % 4, sub)
        k = counter["w"]
        counter["w"] += 1
        send(ref, ref, w_send.at[k], w_recv.at[sem_of(*at)], target[way])

    def across(u, dx, dy):
        ref = unit(u, dx, dy, c)
        k = counter["d"]
        counter["d"] += 1
        send(ref, ref, d_send.at[k], d_recv.at[sem_of(u, dx, dy)], target[CP])

    def piece_in(u, dx, dy, sub=None):
        arrived(unit(u, dx, dy, c, sub), w_recv.at[sem_of(u, dx, dy, sub)])

    def peer_in(u, dx):
        for dy in range(4):
            if (u, dx, dy) not in ((0, 0, 0), (1, 0, 0), (2, 0, 0)):
                arrived(unit(u, dx, dy, 1 - c), d_recv.at[sem_of(u, dx, dy)])

    for u in (0, 1, 2):
        for way in (XP, YP, YM):
            pass_on(u, 0, 0, way)
        send(away.at[:, COLS[u]], w.at[own_rows, COLS[u]], w_send.at[45 + u], w_recv.at[sem_of(3 + u, 0, 0)], target[ZP])
    send(ht.at[z, mine], ht.at[z, mine], h_send.at[15], h_recv.at[1], across_x)
    send(w.at[own_rows], w.at[own_rows], d_send.at[47], d_recv.at[0], target[CP])
    tell(0, along_z(1), along_z(15))
    climb(mrun, mgot, m_send, m_recv, 0)

    fetches[4].wait()

    def fold(block, how):
        return how(block.reshape(16, 8, 128), axis=0)

    def tile(j):
        return slice(j * 128, j * 128 + 128)

    low8 = jnp.full((8, 128), -jnp.inf, F32)
    zero8 = jnp.zeros((8, 128), F32)
    top = low8
    for j in range(NT):
        block = tea_ref[:, tile(j)].astype(F32).T
        tt[tile(j), :] = block
        top = jnp.maximum(top, fold(block, jnp.max))
    t_max = top.max(axis=0, keepdims=True)
    pl.semaphore_wait(ready.at[0], 2)
    tell(1, along_z(2), along_z(14))

    total = zero8
    for j in range(NT):
        e = jnp.exp(tt[tile(j), :] - t_max)
        et[tile(j), :] = e
        total = total + fold(e, jnp.sum)
    t_sum = total.sum(axis=0, keepdims=True)
    tstat[v] = jnp.concatenate([t_max, t_sum], axis=0)
    climb(mrun, mgot, m_send, m_recv, 1)

    hidden = iter(range(15))

    def spread(source, *steps):
        for k in steps:
            rsem = {4: 2, 12: 3}.get(k, 0) if source is z else 0
            send(ht.at[source], ht.at[source], h_send.at[next(hidden)], h_recv.at[rsem], along_z(k))

    arrived(ht.at[z, theirs], h_recv.at[1])
    spread(z, 1, 15, 2, 14)
    pl.semaphore_wait(ready.at[1], 2)
    tell(2, along_z(4), along_z(12))
    spread(z, 3, 13, 4, 12)

    piece_in(0, 0, 3)
    pass_on(0, 0, 3, YP)
    across(0, 0, 3)
    piece_in(0, 0, 1)
    across(0, 0, 1)
    piece_in(3, 0, 0)
    pass_on(3, 0, 0, XP)
    pass_on(3, 0, 0, YP)
    pass_on(3, 0, 0, YM)
    pass_on(0, 0, 3, XP, sub=1)
    pass_on(0, 0, 1, XP, sub=0)
    across(3, 0, 0)
    piece_in(0, 1, 0)
    across(0, 1, 0)
    climb(mrun, mgot, m_send, m_recv, 2)
    for u in (1, 2):
        piece_in(u, 0, 1)
        pass_on(u, 0, 1, YM)
        across(u, 0, 1)
        piece_in(u, 0, 3)
        across(u, 0, 3)
    for u in (4, 5):
        piece_in(u, 0, 0)
        pass_on(u, 0, 0, YP)
        pass_on(u, 0, 0, YM)
        pass_on(u, 0, 0, XP)
        across(u, 0, 0)
    for u in (1, 2):
        piece_in(u, 1, 0)
        across(u, 1, 0)
    piece_in(0, 0, 2)
    pass_on(0, 0, 2, XP)
    across(0, 0, 2)
    piece_in(3, 0, 1)
    across(3, 0, 1)
    piece_in(3, 1, 0)
    across(3, 1, 0)
    climb(mrun, mgot, m_send, m_recv, 3)
    piece_in(3, 0, 3)
    pass_on(3, 0, 3, YP)
    across(3, 0, 3)
    for u in (1, 2):
        piece_in(u, 0, 2)
        pass_on(u, 0, 2, XP)
        across(u, 0, 2)
    before, after = (z + 12) % NZ, (z + 4) % NZ
    arrived(ht.at[before], h_recv.at[2])
    spread(before, 4, 3, 2, 1)
    arrived(ht.at[after], h_recv.at[3])
    spread(after, 13, 14, 15)
    for u in (4, 5):
        piece_in(u, 0, 1)
        pass_on(u, 0, 1, YM)
        across(u, 0, 1)
    for u in (0, 1, 2, 3):
        pass_on(u, 1, 0, YP, sub=None if u else 0)
        pass_on(u, 1, 0, YM, sub=None if u else 1)
    for u in (4, 5):
        piece_in(u, 0, 3)
        across(u, 0, 3)
    for u in (4, 5):
        piece_in(u, 1, 0)
        pass_on(u, 1, 0, YP)
        pass_on(u, 1, 0, YM)
        across(u, 1, 0)
    for u in (3, 4, 5):
        piece_in(u, 0, 2)
        pass_on(u, 0, 2, XP)
        across(u, 0, 2)
    piece_in(0, 1, 2)
    across(0, 1, 2)
    climb(mrun, mgot, m_send, m_recv, 4)
    pl.semaphore_wait(ready.at[2], 2)
    tell(3, across_x)

    arrived(ht.at[pl.ds(0, 13)], h_recv.at[0])
    for g in range(4):
        part = ht[8 * (g % 2) : 8 * (g % 2) + 8, (g // 2) * R : (g // 2) * R + R, :]
        hg[g] = part.reshape(512, TOK).astype(F32).T.astype(BF16)

    def multiply(u, dx):
        g = (h ^ (u // 3)) * 2 + (xl ^ dx)
        rows = pl.ds(pl.multiple_of(g * 512, 512), 512)
        cols = COLS[u % 3]
        part = jnp.dot(hg[g], w[rows, cols], preferred_element_type=F32)
        acc[:, cols] = part if (u // 3, dx) == (0, 0) else acc[:, cols] + part

    def statistics(p):
        top, hit = low8, zero8
        for j in TILES[p]:
            block = acc[:, tile(j)].T
            lt[tile(j), :] = block
            column = lax.broadcasted_iota(jnp.int32, (128, 128), 0) + (v * VT + j * 128)
            top = jnp.maximum(top, fold(block, jnp.max))
            hit = hit + fold(jnp.where(column == ids, block, 0.0), jnp.sum)
        high = top.max(axis=0, keepdims=True)
        total, cross = zero8, zero8
        for j in TILES[p]:
            logit = lt[tile(j), :]
            e = jnp.exp(logit - high)
            lt[tile(j), :] = e
            total = total + fold(e, jnp.sum)
            cross = cross + fold(et[tile(j), :] * (tt[tile(j), :] - logit), jnp.sum)
        return high, *(a.sum(axis=0, keepdims=True) for a in (total, cross, hit))

    fetches[5].wait()
    ids = ids_ref[...]
    other_rows = pl.ds(pl.multiple_of(h * 1024 + R * (d ^ 1), R), R)
    arrived(w.at[other_rows], d_recv.at[0])
    for u in (0, 1, 2):
        peer_in(u, 0)
        multiply(u, 0)
    everybody = []
    for offset in far + [0]:
        for other in (1, 0):
            if other or offset:
                everybody.append(dev(d, (xh ^ other) * NZ + (z + offset) % NZ))
    pl.semaphore_wait(ready.at[3], 1)
    for k, to in enumerate(everybody):
        send(tstat.at[v], tstat.at[v], t_send.at[k], t_recv, to)
    for dy in (3, 1):
        for sub in (0, 1):
            piece_in(0, 1, dy, sub)
        across(0, 1, dy)
    for u in (3, 4, 5):
        peer_in(u, 0)
        multiply(u, 0)
    for u in (1, 2):
        for dy in (2, 3, 1):
            piece_in(u, 1, dy)
            across(u, 1, dy)
    peer_in(0, 1)
    multiply(0, 1)
    for dy in (2, 3, 1):
        piece_in(3, 1, dy)
        across(3, 1, dy)
    for u in (1, 2):
        peer_in(u, 1)
        multiply(u, 1)
    for u in (4, 5):
        piece_in(u, 1, 2)
        across(u, 1, 2)
    peer_in(3, 1)
    multiply(3, 1)
    parts = [statistics(0)]
    for u in (4, 5):
        for dy in (3, 1):
            piece_in(u, 1, dy)
            across(u, 1, dy)
    for u in (4, 5):
        peer_in(u, 1)
        multiply(u, 1)
        parts.append(statistics(u - 3))
    maxima = [part[0] for part in parts]
    s_max = jnp.maximum(jnp.maximum(maxima[0], maxima[1]), maxima[2])
    s_sum = sum(part[1] * jnp.exp(part[0] - s_max) for part in parts)
    x_sum = sum(part[2] for part in parts)
    s_hit = sum(part[3] for part in parts)
    stat[v] = jnp.concatenate([s_max, s_sum, x_sum, s_hit], axis=0)
    for k, to in enumerate(everybody):
        send(stat.at[v], stat.at[v], s_send.at[k], s_recv, to)
    arrived(tstat.at[pl.ds(0, 31)], t_recv)
    count = jnp.sum(mrun[4], axis=1, keepdims=True)
    factor = mask_ref[...].astype(F32) / count
    t_top = tstat[0][0:1]
    for r in range(1, 32):
        t_top = jnp.maximum(t_top, tstat[r][0:1])
    t_scales = [jnp.exp(tstat[r][0:1] - t_top) for r in range(32)]
    tz = sum(t_scales[r] * tstat[r][1:2] for r in range(32))
    t_lse = t_top + jnp.log(tz)
    t_scale = factor * (jnp.exp(t_max - t_top) / tz)
    arrived(stat.at[pl.ds(0, 31)], s_recv)
    tops = stat[0][0:1]
    for r in range(1, 32):
        tops = jnp.maximum(tops, stat[r][0:1])
    xz = sz = hz = jnp.zeros((1, 128), F32)
    for r in range(32):
        one = stat[r]
        sz = sz + jnp.exp(one[0:1] - tops) * one[1:2]
        xz = xz + t_scales[r] * one[2:3]
        hz = hz + one[3:4]
    s_lse = tops + jnp.log(sz)
    kl = xz / tz - t_lse + s_lse
    row_ref[0:1] = kl
    row_ref[1:2] = hz - s_lse
    lrun[0] = kl * mask_ref[...].astype(F32)
    climb(lrun, lgot, l_send, l_recv, 0)

    for p, high in enumerate(maxima):
        s_scale = factor * (jnp.exp(high - tops) / sz)
        for j in TILES[p]:
            dl[tile(j), :] = (lt[tile(j), :] * s_scale - et[tile(j), :] * t_scale).astype(BF16)

    def quarter(half, q):
        rows = pl.ds(pl.multiple_of(half * 1024 + q * 256, 256), 256)
        return jnp.dot(w[rows, :], dl[...], preferred_element_type=F32)

    zq = z // 4
    first, second = 2 * ((3 - zq) // 3), 3 - 2 * (zq // 2)
    order = (first, second, 6 - first - second - zq, zq)
    for i, q in enumerate(order):
        xsend[i] = quarter(1 - xh, q).astype(BF16)
        send(xsend.at[i], xrecv.at[i], x_send.at[i], x_recv.at[i], across_x)
    climb(lrun, lgot, l_send, l_recv, 1)
    for i, q in enumerate(order):
        own[i] = quarter(xh, q)
    climb(lrun, lgot, l_send, l_recv, 2)
    k = 0
    for i, q in enumerate(order):
        arrived(xrecv.at[i], x_recv.at[i])
        both = own[i] + xrecv[i].astype(F32)
        own[i] = both
        zsend[i] = both.astype(BF16)
        for r in range(4) if i < 3 else (2, 3, 1):
            zt = q * 4 + r if i < 3 else z ^ r
            piece = zsend.at[i, pl.ds(pl.multiple_of((zt % 4) * R, R), R)]
            send(piece, zrecv.at[z], z_send.at[k], z_recv, dev(d, xh * NZ + zt))
            k += 1

    climb(lrun, lgot, l_send, l_recv, 3)
    climb(lrun, lgot, l_send, l_recv, 4)
    loss = jnp.sum(lrun[4], axis=1, keepdims=True) / count
    row_ref[2:3] = jnp.broadcast_to(loss, (1, TOK))

    kept = own[3, pl.ds(pl.multiple_of((z % 4) * R, R), R), :]
    arrived(zrecv.at[pl.ds(0, 15)], z_recv)
    for r in range(1, 16):
        kept = kept + zrecv[z ^ r].astype(F32)
    grad_ref[...] = kept.astype(BF16)
    for copy in started:
        copy.wait_send()


def place(grad_in, row_in, grad_ref, kl_ref, samp_ref, loss_ref):
    grad_ref[...] = grad_in[...]
    kl_ref[...] = row_in[0]
    samp_ref[...] = row_in[1]
    loss_ref[...] = row_in[2:3, 0:1]


def on_device(hidden, blocks, teacher, ids, mask):
    vm = pl.BlockSpec(memory_space=pltpu.VMEM)
    hbm = pl.BlockSpec(memory_space=pl.ANY)
    dma = pltpu.SemaphoreType.DMA
    grad, rows = pl.pallas_call(
        kernel,
        out_shape=(jax.ShapeDtypeStruct((R, TOK), BF16), jax.ShapeDtypeStruct((8, TOK), F32)),
        in_specs=[hbm] * 5,
        out_specs=(vm, vm),
        scratch_shapes=[
            pltpu.VMEM((D, VT), BF16),
            pltpu.VMEM((NZ, 2 * R, TOK), BF16),
            pltpu.VMEM((4, TOK, 512), BF16),
            pltpu.VMEM((TOK, VT), F32),
            pltpu.VMEM((VT, TOK), F32),
            pltpu.VMEM((VT, TOK), F32),
            pltpu.VMEM((VT, TOK), F32),
            pltpu.VMEM((VT, TOK), BF16),
            pltpu.VMEM((32, 4, TOK), F32),
            pltpu.VMEM((32, 2, TOK), F32),
            pltpu.VMEM((R, VT), BF16),
            pltpu.VMEM((5, 1, TOK), F32),
            pltpu.VMEM((4, 1, TOK), F32),
            pltpu.VMEM((5, 1, TOK), F32),
            pltpu.VMEM((4, 1, TOK), F32),
            pltpu.VMEM((4, 256, TOK), BF16),
            pltpu.VMEM((4, 256, TOK), BF16),
            pltpu.VMEM((4, 256, TOK), F32),
            pltpu.VMEM((4, 256, TOK), BF16),
            pltpu.VMEM((NZ, R, TOK), BF16),
            pltpu.VMEM((TOK, VT), BF16),
            pltpu.VMEM((1, TOK), jnp.int32),
            pltpu.VMEM((1, TOK), jnp.int32),
            dma((48,)), dma((50,)), dma((48,)), dma((48,)), dma((6,)), dma((16,)), dma((4,)),
            dma((31,)), dma, dma((31,)), dma, dma((4,)), dma((4,)), dma((4,)), dma((4,)), dma((4,)), dma((4,)), dma((16,)), dma,
            pltpu.SemaphoreType.REGULAR((4,)),
        ],
        compiler_params=pltpu.CompilerParams(
            collective_id=0, has_side_effects=True, vmem_limit_bytes=60 * 1024 * 1024
        ),
    )(hidden.T, blocks.reshape(R, 2 * VT), teacher, ids.reshape(1, TOK), mask.reshape(1, TOK))
    grad, kl, samp, loss = pl.pallas_call(
        place,
        out_shape=(
            jax.ShapeDtypeStruct((R, TOK), BF16),
            jax.ShapeDtypeStruct((TOK,), F32),
            jax.ShapeDtypeStruct((TOK,), F32),
            jax.ShapeDtypeStruct((1, 1), F32),
        ),
        in_specs=[vm, vm],
        out_specs=(vm, vm, vm, vm),
    )(grad, rows)
    return grad.T, kl, samp, loss.reshape(())


def solution(mesh):
    return jax.shard_map(
        on_device,
        mesh=mesh,
        in_specs=(P("dp", "vocab"), P("vocab", "dp", None), P("dp", "vocab"), P("dp"), P("dp")),
        out_specs=(P("dp", "vocab"), P("dp"), P("dp"), P()),
        check_vma=False,
    )
```

```python
import jax
import jax.numpy as jnp
from jax import lax
from jax.experimental import pallas as pl
from jax.experimental.pallas import tpu as pltpu
from jax.sharding import PartitionSpec as P

F32 = jnp.float32
BF16 = jnp.bfloat16
D = 2048
VT = 2432
TOK = 128
R = 64
NT = VT // 128
CUTS = (0, 1280, 2048, VT)
COLS = tuple(pl.ds(a, b - a) for a, b in zip(CUTS, CUTS[1:]))
TILES = tuple(range(a // 128, b // 128) for a, b in zip(CUTS, CUTS[1:]))
NZ = 16
MESH = pl.DeviceIdType.MESH

XP, YP, YM, ZP, CP = range(5)


def kernel(
    hid_hbm, blk_ref, tea_hbm, ids_hbm, mask_hbm,
    grad_ref, row_ref,
    w, ht, hg, acc, lt, tt, et, dl, stat, tstat, away, mrun, mgot, lrun, lgot, xsend, xrecv, own, zsend, zrecv, feed, zagg,
    tea_ref, ids_ref, mask_ref,
    w_send, w_recv, d_send, d_recv, loc_sem, h_send, h_recv,
    s_send, s_recv, t_send, t_recv, m_send, m_recv, l_send, l_recv, x_send, x_recv, z_send, z_recv, f_recv, ready,
):
    d = lax.axis_index("dp")
    v = lax.axis_index("vocab")
    xl, y, c = d // 8, (d // 2) % 4, d % 2
    xh, z = v // NZ, v % NZ
    h = v % 2

    def dev(dp, vocab):
        return {"dp": dp, "vocab": vocab}

    def along_z(k):
        return dev(d, xh * NZ + (z + k) % NZ)

    target = {
        XP: dev(d ^ 8, v),
        YP: dev(xl * 8 + ((y + 1) % 4) * 2 + c, v),
        YM: dev(xl * 8 + ((y + 3) % 4) * 2 + c, v),
        ZP: dev(d, v ^ 1),
        CP: dev(d ^ 1, v),
    }
    across_x = dev(d, v ^ NZ)
    ladder = [target[CP], target[XP], dev(xl * 8 + (y ^ 1) * 2 + c, v), dev(xl * 8 + (3 - y) * 2 + c, v)]
    far = [8, 7, 9, 6, 10, 5, 11, 4, 12, 3, 13, 2, 14, 1, 15]
    mine = pl.ds(pl.multiple_of(xh * R, R), R)
    theirs = pl.ds(pl.multiple_of((1 - xh) * R, R), R)

    barrier = pltpu.get_barrier_semaphore()
    for to in (target[YP], target[YM], target[XP], target[CP], along_z(1), along_z(15), across_x):
        pl.semaphore_signal(barrier, inc=1, device_id=to, device_id_type=MESH)
    near = blk_ref.at[:, pl.ds(pl.multiple_of(h * VT, 128), VT)]
    rest = blk_ref.at[:, pl.ds(pl.multiple_of((1 - h) * VT, 128), VT)]
    own_rows = pl.ds(pl.multiple_of(h * 1024 + R * d, R), R)
    fetches = [
        pltpu.make_async_copy(src, dst, loc_sem.at[i])
        for i, (src, dst) in enumerate(
            [
                (near, w.at[own_rows]),
                (rest, away),
                (hid_hbm, ht.at[z, mine]),
                (mask_hbm, mask_ref),
                (tea_hbm, tea_ref),
                (ids_hbm, ids_ref),
            ]
        )
    ]
    for fetch in fetches:
        fetch.start()
    fetches[3].wait()
    mrun[0] = mask_ref[...].astype(F32)
    for fetch in fetches[:3]:
        fetch.wait()
    pl.semaphore_wait(barrier, 7)

    started = []

    def send(src, dst, ssem, rsem, to):
        copy = pltpu.make_async_remote_copy(
            src_ref=src, dst_ref=dst, send_sem=ssem, recv_sem=rsem, device_id=to, device_id_type=MESH
        )
        copy.start()
        started.append(copy)

    def arrived(dst, sem):
        pltpu.make_async_copy(dst, dst, sem).wait()

    def tell(i, *to):
        for device in to:
            pl.semaphore_signal(ready.at[i], inc=1, device_id=device, device_id_type=MESH)

    def climb(run, got, ssem, rsem, step):
        if step:
            arrived(got.at[step - 1], rsem.at[step - 1])
            run[step] = run[step - 1] + got[step - 1]
        if step < 4:
            send(run.at[step], got.at[step], ssem.at[step], rsem.at[step], ladder[step])

    def unit(u, dx, dy, core, sub=None):
        base = (h ^ (u // 3)) * 1024 + R * ((xl ^ dx) * 8 + ((y + dy) % 4) * 2 + core)
        if sub is None:
            return w.at[pl.ds(pl.multiple_of(base, R), R), COLS[u % 3]]
        return w.at[pl.ds(pl.multiple_of(base + 32 * sub, 32), 32), COLS[u % 3]]

    counter = {"w": 0, "d": 0}
    subs = {(0, 1, 1, 0): 48, (0, 1, 3, 1): 49, (0, 1, 1, 1): None, (0, 1, 3, 0): None}

    def sem_of(u, dx, dy, sub=None):
        return subs.get((u, dx, dy, sub)) or u * 8 + dx * 4 + dy

    def pass_on(u, dx, dy, way, sub=None):
        ref = unit(u, dx, dy, c, sub)
        if way == XP:
            at = (u, dx ^ 1, dy, sub)
        elif way == YP:
            at = (u, dx, (dy + 3) % 4, sub)
        elif way == YM:
            at = (u, dx, (dy + 1) % 4, sub)
        k = counter["w"]
        counter["w"] += 1
        send(ref, ref, w_send.at[k], w_recv.at[sem_of(*at)], target[way])

    def across(u, dx, dy):
        ref = unit(u, dx, dy, c)
        k = counter["d"]
        counter["d"] += 1
        send(ref, ref, d_send.at[k], d_recv.at[sem_of(u, dx, dy)], target[CP])

    def piece_in(u, dx, dy, sub=None):
        arrived(unit(u, dx, dy, c, sub), w_recv.at[sem_of(u, dx, dy, sub)])

    def peer_in(u, dx):
        for dy in range(4):
            if (u, dx, dy) not in ((0, 0, 0), (1, 0, 0), (2, 0, 0)):
                arrived(unit(u, dx, dy, 1 - c), d_recv.at[sem_of(u, dx, dy)])

    for u in (0, 1, 2):
        for way in (XP, YP, YM):
            pass_on(u, 0, 0, way)
        send(away.at[:, COLS[u]], w.at[own_rows, COLS[u]], w_send.at[45 + u], w_recv.at[sem_of(3 + u, 0, 0)], target[ZP])
    send(ht.at[z, mine], ht.at[z, mine], h_send.at[15], h_recv.at[1], across_x)
    send(w.at[own_rows], w.at[own_rows], d_send.at[47], d_recv.at[0], target[CP])
    tell(0, along_z(1), along_z(15))
    climb(mrun, mgot, m_send, m_recv, 0)

    fetches[4].wait()

    def fold(block, how):
        return how(block.reshape(16, 8, 128), axis=0)

    def tile(j):
        return slice(j * 128, j * 128 + 128)

    low8 = jnp.full((8, 128), -jnp.inf, F32)
    zero8 = jnp.zeros((8, 128), F32)
    top = low8
    for j in range(NT):
        block = tea_ref[:, tile(j)].astype(F32).T
        tt[tile(j), :] = block
        top = jnp.maximum(top, fold(block, jnp.max))
    t_max = top.max(axis=0, keepdims=True)
    pl.semaphore_wait(ready.at[0], 2)
    tell(1, along_z(2), along_z(14))

    total = zero8
    for j in range(NT):
        e = jnp.exp(tt[tile(j), :] - t_max)
        et[tile(j), :] = e
        total = total + fold(e, jnp.sum)
    t_sum = total.sum(axis=0, keepdims=True)
    tstat[v] = jnp.concatenate([t_max, t_sum], axis=0)
    climb(mrun, mgot, m_send, m_recv, 1)

    hidden = iter(range(15))

    def spread(source, *steps):
        for k in steps:
            rsem = {4: 2, 12: 3}.get(k, 0) if source is z else 0
            send(ht.at[source], ht.at[source], h_send.at[next(hidden)], h_recv.at[rsem], along_z(k))

    arrived(ht.at[z, theirs], h_recv.at[1])
    spread(z, 1, 15, 2, 14)
    pl.semaphore_wait(ready.at[1], 2)
    tell(2, along_z(4), along_z(12))
    spread(z, 3, 13, 4, 12)

    piece_in(0, 0, 3)
    pass_on(0, 0, 3, YP)
    across(0, 0, 3)
    piece_in(0, 0, 1)
    across(0, 0, 1)
    piece_in(3, 0, 0)
    pass_on(3, 0, 0, XP)
    pass_on(3, 0, 0, YP)
    pass_on(3, 0, 0, YM)
    pass_on(0, 0, 3, XP, sub=1)
    pass_on(0, 0, 1, XP, sub=0)
    across(3, 0, 0)
    piece_in(0, 1, 0)
    across(0, 1, 0)
    climb(mrun, mgot, m_send, m_recv, 2)
    for u in (1, 2):
        piece_in(u, 0, 1)
        pass_on(u, 0, 1, YM)
        across(u, 0, 1)
        piece_in(u, 0, 3)
        across(u, 0, 3)
    for u in (4, 5):
        piece_in(u, 0, 0)
        pass_on(u, 0, 0, YP)
        pass_on(u, 0, 0, YM)
        pass_on(u, 0, 0, XP)
        across(u, 0, 0)
    for u in (1, 2):
        piece_in(u, 1, 0)
        across(u, 1, 0)
    piece_in(0, 0, 2)
    pass_on(0, 0, 2, XP)
    across(0, 0, 2)
    piece_in(3, 0, 1)
    across(3, 0, 1)
    piece_in(3, 1, 0)
    across(3, 1, 0)
    climb(mrun, mgot, m_send, m_recv, 3)
    piece_in(3, 0, 3)
    pass_on(3, 0, 3, YP)
    across(3, 0, 3)
    for u in (1, 2):
        piece_in(u, 0, 2)
        pass_on(u, 0, 2, XP)
        across(u, 0, 2)
    before, after = (z + 12) % NZ, (z + 4) % NZ
    arrived(ht.at[before], h_recv.at[2])
    spread(before, 4, 3, 2, 1)
    arrived(ht.at[after], h_recv.at[3])
    spread(after, 13, 14, 15)
    for u in (4, 5):
        piece_in(u, 0, 1)
        pass_on(u, 0, 1, YM)
        across(u, 0, 1)
    for u in (0, 1, 2, 3):
        pass_on(u, 1, 0, YP, sub=None if u else 0)
        pass_on(u, 1, 0, YM, sub=None if u else 1)
    for u in (4, 5):
        piece_in(u, 0, 3)
        across(u, 0, 3)
    for u in (4, 5):
        piece_in(u, 1, 0)
        pass_on(u, 1, 0, YP)
        pass_on(u, 1, 0, YM)
        across(u, 1, 0)
    for u in (3, 4, 5):
        piece_in(u, 0, 2)
        pass_on(u, 0, 2, XP)
        across(u, 0, 2)
    piece_in(0, 1, 2)
    across(0, 1, 2)
    climb(mrun, mgot, m_send, m_recv, 4)
    pl.semaphore_wait(ready.at[2], 2)
    tell(3, across_x)

    arrived(ht.at[pl.ds(0, 13)], h_recv.at[0])
    for g in range(4):
        part = ht[8 * (g % 2) : 8 * (g % 2) + 8, (g // 2) * R : (g // 2) * R + R, :]
        hg[g] = part.reshape(512, TOK).astype(F32).T.astype(BF16)

    def multiply(u, dx):
        g = (h ^ (u // 3)) * 2 + (xl ^ dx)
        rows = pl.ds(pl.multiple_of(g * 512, 512), 512)
        cols = COLS[u % 3]
        part = jnp.dot(hg[g], w[rows, cols], preferred_element_type=F32)
        acc[:, cols] = part if (u // 3, dx) == (0, 0) else acc[:, cols] + part

    def statistics(p):
        top, hit = low8, zero8
        for j in TILES[p]:
            block = acc[:, tile(j)].T
            lt[tile(j), :] = block
            column = lax.broadcasted_iota(jnp.int32, (128, 128), 0) + (v * VT + j * 128)
            top = jnp.maximum(top, fold(block, jnp.max))
            hit = hit + fold(jnp.where(column == ids, block, 0.0), jnp.sum)
        high = top.max(axis=0, keepdims=True)
        total, cross = zero8, zero8
        for j in TILES[p]:
            logit = lt[tile(j), :]
            e = jnp.exp(logit - high)
            lt[tile(j), :] = e
            total = total + fold(e, jnp.sum)
            cross = cross + fold(et[tile(j), :] * (tt[tile(j), :] - logit), jnp.sum)
        return high, *(a.sum(axis=0, keepdims=True) for a in (total, cross, hit))

    fetches[5].wait()
    ids = ids_ref[...]
    other_rows = pl.ds(pl.multiple_of(h * 1024 + R * (d ^ 1), R), R)
    arrived(w.at[other_rows], d_recv.at[0])
    for u in (0, 1, 2):
        peer_in(u, 0)
        multiply(u, 0)
    everybody = []
    for offset in far + [0]:
        for other in (1, 0):
            if other or offset:
                everybody.append(dev(d, (xh ^ other) * NZ + (z + offset) % NZ))
    pl.semaphore_wait(ready.at[3], 1)
    for k, to in enumerate(everybody):
        send(tstat.at[v], tstat.at[v], t_send.at[k], t_recv, to)
    for dy in (3, 1):
        for sub in (0, 1):
            piece_in(0, 1, dy, sub)
        across(0, 1, dy)
    for u in (3, 4, 5):
        peer_in(u, 0)
        multiply(u, 0)
    for u in (1, 2):
        for dy in (2, 3, 1):
            piece_in(u, 1, dy)
            across(u, 1, dy)
    peer_in(0, 1)
    multiply(0, 1)
    for dy in (2, 3, 1):
        piece_in(3, 1, dy)
        across(3, 1, dy)
    for u in (1, 2):
        peer_in(u, 1)
        multiply(u, 1)
    for u in (4, 5):
        piece_in(u, 1, 2)
        across(u, 1, 2)
    peer_in(3, 1)
    multiply(3, 1)
    parts = [statistics(0)]
    for u in (4, 5):
        for dy in (3, 1):
            piece_in(u, 1, dy)
            across(u, 1, dy)
    for u in (4, 5):
        peer_in(u, 1)
        multiply(u, 1)
        parts.append(statistics(u - 3))
    maxima = [part[0] for part in parts]
    s_max = jnp.maximum(jnp.maximum(maxima[0], maxima[1]), maxima[2])
    s_sum = sum(part[1] * jnp.exp(part[0] - s_max) for part in parts)
    x_sum = sum(part[2] for part in parts)
    s_hit = sum(part[3] for part in parts)
    stat[v] = jnp.concatenate([s_max, s_sum, x_sum, s_hit], axis=0)
    for k, to in enumerate(everybody):
        send(stat.at[v], stat.at[v], s_send.at[k], s_recv, to)
    arrived(tstat.at[pl.ds(0, 31)], t_recv)
    count = jnp.sum(mrun[4], axis=1, keepdims=True)
    factor = mask_ref[...].astype(F32) / count
    t_top = tstat[0][0:1]
    for r in range(1, 32):
        t_top = jnp.maximum(t_top, tstat[r][0:1])
    t_scales = [jnp.exp(tstat[r][0:1] - t_top) for r in range(32)]
    tz = sum(t_scales[r] * tstat[r][1:2] for r in range(32))
    t_lse = t_top + jnp.log(tz)
    t_scale = factor * (jnp.exp(t_max - t_top) / tz)
    arrived(stat.at[pl.ds(0, 31)], s_recv)
    tops = stat[0][0:1]
    for r in range(1, 32):
        tops = jnp.maximum(tops, stat[r][0:1])
    xz = sz = hz = jnp.zeros((1, 128), F32)
    for r in range(32):
        one = stat[r]
        sz = sz + jnp.exp(one[0:1] - tops) * one[1:2]
        xz = xz + t_scales[r] * one[2:3]
        hz = hz + one[3:4]
    s_lse = tops + jnp.log(sz)
    kl = xz / tz - t_lse + s_lse
    row_ref[0:1] = kl
    row_ref[1:2] = hz - s_lse
    lrun[0] = kl * mask_ref[...].astype(F32)
    climb(lrun, lgot, l_send, l_recv, 0)

    for p, high in enumerate(maxima):
        s_scale = factor * (jnp.exp(high - tops) / sz)
        for j in TILES[p]:
            dl[tile(j), :] = (lt[tile(j), :] * s_scale - et[tile(j), :] * t_scale).astype(BF16)

    groups = ((8, 7, 9, 6), (10, 5, 11, 4), (12, 3, 13, 2), (14, 1, 15, 0))
    feeds = {8: (4, 0), 7: (3, 1), 6: (2, 2), 5: (1, 3), 9: (13, 4), 10: (14, 5), 11: (15, 6)}
    slots = {4: 0, 12: 1, 3: 2, 13: 3, 2: 4, 14: 5, 1: 6, 15: 7}

    def blocks_of(half, group):
        lines = [w[pl.ds(pl.multiple_of(half * 1024 + ((z + k) % NZ) * R, R), R), :] for k in group]
        return jnp.dot(jnp.concatenate(lines, axis=0), dl[...], preferred_element_type=F32)

    for i, group in enumerate(groups):
        xsend[i] = blocks_of(1 - xh, group).astype(BF16)
        send(xsend.at[i], xrecv.at[i], x_send.at[i], x_recv.at[i], across_x)
    climb(lrun, lgot, l_send, l_recv, 1)
    for i, group in enumerate(groups):
        own[i] = blocks_of(xh, group)
    links = iter(range(15))
    for i, group in enumerate(groups):
        arrived(xrecv.at[i], x_recv.at[i])
        both = own[i] + xrecv[i].astype(F32)
        own[i] = both
        zsend[i] = both.astype(BF16)
        for r, step in enumerate(group):
            piece = zsend.at[i, pl.ds(r * R, R)]
            if step in feeds:
                node, slot = feeds[step]
                send(piece, feed.at[slot], z_send.at[next(links)], f_recv.at[slot // 4], along_z(node))
            elif step not in (0, 4, 12):
                send(piece, zrecv.at[slots[step]], z_send.at[next(links)], z_recv, along_z(step))
        if i == 1:
            climb(lrun, lgot, l_send, l_recv, 2)
    for side, (step, kept, count_in) in enumerate(((4, own[1, 3 * R :, :], 4), (12, own[2, :R, :], 3))):
        arrived(feed.at[pl.ds(4 * side, count_in)], f_recv.at[side])
        for slot in range(count_in):
            kept = kept + feed[4 * side + slot].astype(F32)
        zagg[side] = kept.astype(BF16)
        send(zagg.at[side], zrecv.at[slots[step]], z_send.at[next(links)], z_recv, along_z(step))

    climb(lrun, lgot, l_send, l_recv, 3)
    kept = own[3, 3 * R :, :]
    arrived(zrecv, z_recv)
    for slot in range(8):
        kept = kept + zrecv[slot].astype(F32)
    grad_ref[...] = kept.astype(BF16)
    climb(lrun, lgot, l_send, l_recv, 4)
    loss = jnp.sum(lrun[4], axis=1, keepdims=True) / count
    row_ref[2:3] = jnp.broadcast_to(loss, (1, TOK))
    for copy in started:
        copy.wait_send()


def place(grad_in, row_in, grad_ref, kl_ref, samp_ref, loss_ref):
    grad_ref[...] = grad_in[...]
    kl_ref[...] = row_in[0]
    samp_ref[...] = row_in[1]
    loss_ref[...] = row_in[2:3, 0:1]


def on_device(hidden, blocks, teacher, ids, mask):
    vm = pl.BlockSpec(memory_space=pltpu.VMEM)
    hbm = pl.BlockSpec(memory_space=pl.ANY)
    dma = pltpu.SemaphoreType.DMA
    grad, rows = pl.pallas_call(
        kernel,
        out_shape=(jax.ShapeDtypeStruct((R, TOK), BF16), jax.ShapeDtypeStruct((8, TOK), F32)),
        in_specs=[hbm] * 5,
        out_specs=(vm, vm),
        scratch_shapes=[
            pltpu.VMEM((D, VT), BF16),
            pltpu.VMEM((NZ, 2 * R, TOK), BF16),
            pltpu.VMEM((4, TOK, 512), BF16),
            pltpu.VMEM((TOK, VT), F32),
            pltpu.VMEM((VT, TOK), F32),
            pltpu.VMEM((VT, TOK), F32),
            pltpu.VMEM((VT, TOK), F32),
            pltpu.VMEM((VT, TOK), BF16),
            pltpu.VMEM((32, 4, TOK), F32),
            pltpu.VMEM((32, 2, TOK), F32),
            pltpu.VMEM((R, VT), BF16),
            pltpu.VMEM((5, 1, TOK), F32),
            pltpu.VMEM((4, 1, TOK), F32),
            pltpu.VMEM((5, 1, TOK), F32),
            pltpu.VMEM((4, 1, TOK), F32),
            pltpu.VMEM((4, 256, TOK), BF16),
            pltpu.VMEM((4, 256, TOK), BF16),
            pltpu.VMEM((4, 256, TOK), F32),
            pltpu.VMEM((4, 256, TOK), BF16),
            pltpu.VMEM((8, R, TOK), BF16),
            pltpu.VMEM((7, R, TOK), BF16),
            pltpu.VMEM((2, R, TOK), BF16),
            pltpu.VMEM((TOK, VT), BF16),
            pltpu.VMEM((1, TOK), jnp.int32),
            pltpu.VMEM((1, TOK), jnp.int32),
            dma((48,)), dma((50,)), dma((48,)), dma((48,)), dma((6,)), dma((16,)), dma((4,)),
            dma((31,)), dma, dma((31,)), dma, dma((4,)), dma((4,)), dma((4,)), dma((4,)), dma((4,)), dma((4,)), dma((16,)), dma, dma((2,)),
            pltpu.SemaphoreType.REGULAR((4,)),
        ],
        compiler_params=pltpu.CompilerParams(
            collective_id=0, has_side_effects=True, vmem_limit_bytes=60 * 1024 * 1024
        ),
    )(hidden.T, blocks.reshape(R, 2 * VT), teacher, ids.reshape(1, TOK), mask.reshape(1, TOK))
    grad, kl, samp, loss = pl.pallas_call(
        place,
        out_shape=(
            jax.ShapeDtypeStruct((R, TOK), BF16),
            jax.ShapeDtypeStruct((TOK,), F32),
            jax.ShapeDtypeStruct((TOK,), F32),
            jax.ShapeDtypeStruct((1, 1), F32),
        ),
        in_specs=[vm, vm],
        out_specs=(vm, vm, vm, vm),
    )(grad, rows)
    return grad.T, kl, samp, loss.reshape(())


def solution(mesh):
    return jax.shard_map(
        on_device,
        mesh=mesh,
        in_specs=(P("dp", "vocab"), P("vocab", "dp", None), P("dp", "vocab"), P("dp"), P("dp")),
        out_specs=(P("dp", "vocab"), P("dp"), P("dp"), P()),
        check_vma=False,
    )
```

```python
import jax
import jax.numpy as jnp
from jax import lax
from jax.experimental import pallas as pl
from jax.experimental.pallas import tpu as pltpu
from jax.sharding import PartitionSpec as P

F32 = jnp.float32
BF16 = jnp.bfloat16
D = 2048
VT = 2432
TOK = 128
R = 64
NT = VT // 128
CUTS = (0, 1280, 2176, VT)
COLS = tuple(pl.ds(a, b - a) for a, b in zip(CUTS, CUTS[1:]))
TILES = tuple(range(a // 128, b // 128) for a, b in zip(CUTS, CUTS[1:]))
NZ = 16
MESH = pl.DeviceIdType.MESH

XP, YP, YM, ZP, CP = range(5)


def kernel(
    hid_hbm, blk_ref, tea_hbm, ids_hbm, mask_hbm,
    grad_ref, row_ref,
    w, ht, hg, acc, lt, tt, et, dl, stat, tstat, away, mrun, mgot, lrun, lgot, xsend, xrecv, own, zsend, zrecv, feed, zagg,
    tea_ref, ids_ref, mask_ref,
    w_send, w_recv, d_send, d_recv, loc_sem, h_send, h_recv,
    s_send, s_recv, t_send, t_recv, m_send, m_recv, l_send, l_recv, x_send, x_recv, z_send, z_recv, f_recv, ready,
):
    d = lax.axis_index("dp")
    v = lax.axis_index("vocab")
    xl, y, c = d // 8, (d // 2) % 4, d % 2
    xh, z = v // NZ, v % NZ
    h = v % 2

    def dev(dp, vocab):
        return {"dp": dp, "vocab": vocab}

    def along_z(k):
        return dev(d, xh * NZ + (z + k) % NZ)

    target = {
        XP: dev(d ^ 8, v),
        YP: dev(xl * 8 + ((y + 1) % 4) * 2 + c, v),
        YM: dev(xl * 8 + ((y + 3) % 4) * 2 + c, v),
        ZP: dev(d, v ^ 1),
        CP: dev(d ^ 1, v),
    }
    across_x = dev(d, v ^ NZ)
    ladder = [target[CP], target[XP], dev(xl * 8 + (y ^ 1) * 2 + c, v), dev(xl * 8 + (3 - y) * 2 + c, v)]
    far = [8, 7, 9, 6, 10, 5, 11, 4, 12, 3, 13, 2, 14, 1, 15]
    mine = pl.ds(pl.multiple_of(xh * R, R), R)
    theirs = pl.ds(pl.multiple_of((1 - xh) * R, R), R)

    barrier = pltpu.get_barrier_semaphore()
    for to in (target[YP], target[YM], target[XP], target[CP], along_z(1), along_z(15), across_x):
        pl.semaphore_signal(barrier, inc=1, device_id=to, device_id_type=MESH)
    near = blk_ref.at[:, pl.ds(pl.multiple_of(h * VT, 128), VT)]
    rest = blk_ref.at[:, pl.ds(pl.multiple_of((1 - h) * VT, 128), VT)]
    own_rows = pl.ds(pl.multiple_of(h * 1024 + R * d, R), R)
    fetches = [
        pltpu.make_async_copy(src, dst, loc_sem.at[i])
        for i, (src, dst) in enumerate(
            [
                (near, w.at[own_rows]),
                (rest, away),
                (hid_hbm, ht.at[z, mine]),
                (mask_hbm, mask_ref),
                (tea_hbm, tea_ref),
                (ids_hbm, ids_ref),
            ]
        )
    ]
    for fetch in fetches:
        fetch.start()
    fetches[3].wait()
    mrun[0] = mask_ref[...].astype(F32)
    for fetch in fetches[:3]:
        fetch.wait()
    pl.semaphore_wait(barrier, 7)

    started = []

    def send(src, dst, ssem, rsem, to):
        copy = pltpu.make_async_remote_copy(
            src_ref=src, dst_ref=dst, send_sem=ssem, recv_sem=rsem, device_id=to, device_id_type=MESH
        )
        copy.start()
        started.append(copy)

    def arrived(dst, sem):
        pltpu.make_async_copy(dst, dst, sem).wait()

    def tell(i, *to):
        for device in to:
            pl.semaphore_signal(ready.at[i], inc=1, device_id=device, device_id_type=MESH)

    def climb(run, got, ssem, rsem, step):
        if step:
            arrived(got.at[step - 1], rsem.at[step - 1])
            run[step] = run[step - 1] + got[step - 1]
        if step < 4:
            send(run.at[step], got.at[step], ssem.at[step], rsem.at[step], ladder[step])

    def unit(u, dx, dy, core, sub=None):
        base = (h ^ (u // 3)) * 1024 + R * ((xl ^ dx) * 8 + ((y + dy) % 4) * 2 + core)
        if sub is None:
            return w.at[pl.ds(pl.multiple_of(base, R), R), COLS[u % 3]]
        return w.at[pl.ds(pl.multiple_of(base + 32 * sub, 32), 32), COLS[u % 3]]

    counter = {"w": 0, "d": 0}
    subs = {(0, 1, 1, 0): 48, (0, 1, 3, 1): 49, (0, 1, 1, 1): None, (0, 1, 3, 0): None}

    def sem_of(u, dx, dy, sub=None):
        return subs.get((u, dx, dy, sub)) or u * 8 + dx * 4 + dy

    def pass_on(u, dx, dy, way, sub=None):
        ref = unit(u, dx, dy, c, sub)
        if way == XP:
            at = (u, dx ^ 1, dy, sub)
        elif way == YP:
            at = (u, dx, (dy + 3) % 4, sub)
        elif way == YM:
            at = (u, dx, (dy + 1) % 4, sub)
        k = counter["w"]
        counter["w"] += 1
        send(ref, ref, w_send.at[k], w_recv.at[sem_of(*at)], target[way])

    def across(u, dx, dy):
        ref = unit(u, dx, dy, c)
        k = counter["d"]
        counter["d"] += 1
        send(ref, ref, d_send.at[k], d_recv.at[sem_of(u, dx, dy)], target[CP])

    def piece_in(u, dx, dy, sub=None):
        arrived(unit(u, dx, dy, c, sub), w_recv.at[sem_of(u, dx, dy, sub)])

    def peer_in(u, dx):
        for dy in range(4):
            if (u, dx, dy) not in ((0, 0, 0), (1, 0, 0), (2, 0, 0)):
                arrived(unit(u, dx, dy, 1 - c), d_recv.at[sem_of(u, dx, dy)])

    for u in (0, 1, 2):
        for way in (XP, YP, YM):
            pass_on(u, 0, 0, way)
        send(away.at[:, COLS[u]], w.at[own_rows, COLS[u]], w_send.at[45 + u], w_recv.at[sem_of(3 + u, 0, 0)], target[ZP])
    send(ht.at[z, mine], ht.at[z, mine], h_send.at[15], h_recv.at[1], across_x)
    send(w.at[own_rows], w.at[own_rows], d_send.at[47], d_recv.at[0], target[CP])
    tell(0, along_z(1), along_z(15))
    climb(mrun, mgot, m_send, m_recv, 0)

    fetches[4].wait()

    def fold(block, how):
        return how(block.reshape(16, 8, 128), axis=0)

    def tile(j):
        return slice(j * 128, j * 128 + 128)

    low8 = jnp.full((8, 128), -jnp.inf, F32)
    zero8 = jnp.zeros((8, 128), F32)
    top = low8
    for j in range(NT):
        block = tea_ref[:, tile(j)].astype(F32).T
        tt[tile(j), :] = block
        top = jnp.maximum(top, fold(block, jnp.max))
    t_max = top.max(axis=0, keepdims=True)
    pl.semaphore_wait(ready.at[0], 2)
    tell(1, along_z(2), along_z(14))

    total = zero8
    for j in range(NT):
        e = jnp.exp(tt[tile(j), :] - t_max)
        et[tile(j), :] = e
        total = total + fold(e, jnp.sum)
    t_sum = total.sum(axis=0, keepdims=True)
    tstat[v] = jnp.concatenate([t_max, t_sum], axis=0)
    climb(mrun, mgot, m_send, m_recv, 1)

    hidden = iter(range(15))

    def spread(source, *steps):
        for k in steps:
            rsem = {4: 2, 12: 3}.get(k, 0) if source is z else 0
            send(ht.at[source], ht.at[source], h_send.at[next(hidden)], h_recv.at[rsem], along_z(k))

    arrived(ht.at[z, theirs], h_recv.at[1])
    spread(z, 1, 15, 2, 14)
    pl.semaphore_wait(ready.at[1], 2)
    tell(2, along_z(4), along_z(12))
    spread(z, 3, 13, 4, 12)

    piece_in(0, 0, 3)
    pass_on(0, 0, 3, YP)
    across(0, 0, 3)
    piece_in(0, 0, 1)
    across(0, 0, 1)
    piece_in(3, 0, 0)
    pass_on(3, 0, 0, XP)
    pass_on(3, 0, 0, YP)
    pass_on(3, 0, 0, YM)
    pass_on(0, 0, 3, XP, sub=1)
    pass_on(0, 0, 1, XP, sub=0)
    across(3, 0, 0)
    piece_in(0, 1, 0)
    across(0, 1, 0)
    climb(mrun, mgot, m_send, m_recv, 2)
    for u in (1, 2):
        piece_in(u, 0, 1)
        pass_on(u, 0, 1, YM)
        across(u, 0, 1)
        piece_in(u, 0, 3)
        across(u, 0, 3)
    for u in (4, 5):
        piece_in(u, 0, 0)
        pass_on(u, 0, 0, YP)
        pass_on(u, 0, 0, YM)
        pass_on(u, 0, 0, XP)
        across(u, 0, 0)
    for u in (1, 2):
        piece_in(u, 1, 0)
        across(u, 1, 0)
    piece_in(0, 0, 2)
    pass_on(0, 0, 2, XP)
    across(0, 0, 2)
    piece_in(3, 0, 1)
    across(3, 0, 1)
    piece_in(3, 1, 0)
    across(3, 1, 0)
    climb(mrun, mgot, m_send, m_recv, 3)
    piece_in(3, 0, 3)
    pass_on(3, 0, 3, YP)
    across(3, 0, 3)
    for u in (1, 2):
        piece_in(u, 0, 2)
        pass_on(u, 0, 2, XP)
        across(u, 0, 2)
    before, after = (z + 12) % NZ, (z + 4) % NZ
    arrived(ht.at[before], h_recv.at[2])
    spread(before, 4, 3, 2, 1)
    arrived(ht.at[after], h_recv.at[3])
    spread(after, 13, 14, 15)
    for u in (4, 5):
        piece_in(u, 0, 1)
        pass_on(u, 0, 1, YM)
        across(u, 0, 1)
    for u in (0, 1, 2, 3):
        pass_on(u, 1, 0, YP, sub=None if u else 0)
        pass_on(u, 1, 0, YM, sub=None if u else 1)
    for u in (4, 5):
        piece_in(u, 0, 3)
        across(u, 0, 3)
    for u in (4, 5):
        piece_in(u, 1, 0)
        pass_on(u, 1, 0, YP)
        pass_on(u, 1, 0, YM)
        across(u, 1, 0)
    for u in (3, 4, 5):
        piece_in(u, 0, 2)
        pass_on(u, 0, 2, XP)
        across(u, 0, 2)
    piece_in(0, 1, 2)
    across(0, 1, 2)
    climb(mrun, mgot, m_send, m_recv, 4)
    pl.semaphore_wait(ready.at[2], 2)
    tell(3, across_x)

    arrived(ht.at[pl.ds(0, 13)], h_recv.at[0])
    for g in range(4):
        part = ht[8 * (g % 2) : 8 * (g % 2) + 8, (g // 2) * R : (g // 2) * R + R, :]
        hg[g] = part.reshape(512, TOK).astype(F32).T.astype(BF16)

    def multiply(u, dx):
        g = (h ^ (u // 3)) * 2 + (xl ^ dx)
        rows = pl.ds(pl.multiple_of(g * 512, 512), 512)
        cols = COLS[u % 3]
        part = jnp.dot(hg[g], w[rows, cols], preferred_element_type=F32)
        acc[:, cols] = part if (u // 3, dx) == (0, 0) else acc[:, cols] + part

    def statistics(p):
        top, hit = low8, zero8
        for j in TILES[p]:
            block = acc[:, tile(j)].T
            lt[tile(j), :] = block
            column = lax.broadcasted_iota(jnp.int32, (128, 128), 0) + (v * VT + j * 128)
            top = jnp.maximum(top, fold(block, jnp.max))
            hit = hit + fold(jnp.where(column == ids, block, 0.0), jnp.sum)
        high = top.max(axis=0, keepdims=True)
        total, cross = zero8, zero8
        for j in TILES[p]:
            logit = lt[tile(j), :]
            e = jnp.exp(logit - high)
            lt[tile(j), :] = e
            total = total + fold(e, jnp.sum)
            cross = cross + fold(et[tile(j), :] * (tt[tile(j), :] - logit), jnp.sum)
        return high, *(a.sum(axis=0, keepdims=True) for a in (total, cross, hit))

    fetches[5].wait()
    ids = ids_ref[...]
    other_rows = pl.ds(pl.multiple_of(h * 1024 + R * (d ^ 1), R), R)
    arrived(w.at[other_rows], d_recv.at[0])
    for u in (0, 1, 2):
        peer_in(u, 0)
        multiply(u, 0)
    everybody = []
    for offset in far + [0]:
        for other in (1, 0):
            if other or offset:
                everybody.append(dev(d, (xh ^ other) * NZ + (z + offset) % NZ))
    pl.semaphore_wait(ready.at[3], 1)
    for k, to in enumerate(everybody):
        send(tstat.at[v], tstat.at[v], t_send.at[k], t_recv, to)
    for dy in (3, 1):
        for sub in (0, 1):
            piece_in(0, 1, dy, sub)
        across(0, 1, dy)
    for u in (3, 4, 5):
        peer_in(u, 0)
        multiply(u, 0)
    for u in (1, 2):
        for dy in (2, 3, 1):
            piece_in(u, 1, dy)
            across(u, 1, dy)
    peer_in(0, 1)
    multiply(0, 1)
    for dy in (2, 3, 1):
        piece_in(3, 1, dy)
        across(3, 1, dy)
    for u in (1, 2):
        peer_in(u, 1)
        multiply(u, 1)
    for u in (4, 5):
        piece_in(u, 1, 2)
        across(u, 1, 2)
    peer_in(3, 1)
    multiply(3, 1)
    parts = [statistics(0)]
    for u in (4, 5):
        for dy in (3, 1):
            piece_in(u, 1, dy)
            across(u, 1, dy)
    for u in (4, 5):
        peer_in(u, 1)
        multiply(u, 1)
        parts.append(statistics(u - 3))
    maxima = [part[0] for part in parts]
    s_max = jnp.maximum(jnp.maximum(maxima[0], maxima[1]), maxima[2])
    s_sum = sum(part[1] * jnp.exp(part[0] - s_max) for part in parts)
    x_sum = sum(part[2] for part in parts)
    s_hit = sum(part[3] for part in parts)
    stat[v] = jnp.concatenate([s_max, s_sum, x_sum, s_hit], axis=0)
    for k, to in enumerate(everybody):
        send(stat.at[v], stat.at[v], s_send.at[k], s_recv, to)
    arrived(tstat.at[pl.ds(0, 31)], t_recv)
    count = jnp.sum(mrun[4], axis=1, keepdims=True)
    factor = mask_ref[...].astype(F32) / count
    t_top = tstat[0][0:1]
    for r in range(1, 32):
        t_top = jnp.maximum(t_top, tstat[r][0:1])
    t_scales = [jnp.exp(tstat[r][0:1] - t_top) for r in range(32)]
    tz = sum(t_scales[r] * tstat[r][1:2] for r in range(32))
    t_lse = t_top + jnp.log(tz)
    t_scale = factor * (jnp.exp(t_max - t_top) / tz)
    arrived(stat.at[pl.ds(0, 31)], s_recv)
    tops = stat[0][0:1]
    for r in range(1, 32):
        tops = jnp.maximum(tops, stat[r][0:1])
    xz = sz = hz = jnp.zeros((1, 128), F32)
    for r in range(32):
        one = stat[r]
        sz = sz + jnp.exp(one[0:1] - tops) * one[1:2]
        xz = xz + t_scales[r] * one[2:3]
        hz = hz + one[3:4]
    s_lse = tops + jnp.log(sz)
    kl = xz / tz - t_lse + s_lse
    row_ref[0:1] = kl
    row_ref[1:2] = hz - s_lse
    lrun[0] = kl * mask_ref[...].astype(F32)
    climb(lrun, lgot, l_send, l_recv, 0)

    for p, high in enumerate(maxima):
        s_scale = factor * (jnp.exp(high - tops) / sz)
        for j in TILES[p]:
            dl[tile(j), :] = (lt[tile(j), :] * s_scale - et[tile(j), :] * t_scale).astype(BF16)

    groups = ((8, 7, 9, 6), (10, 5, 11, 4), (12, 3, 13, 2), (14, 1, 15, 0))
    feeds = {8: (4, 0), 7: (3, 1), 6: (2, 2), 5: (1, 3), 9: (13, 4), 10: (14, 5), 11: (15, 6)}
    slots = {4: 0, 12: 1, 3: 2, 13: 3, 2: 4, 14: 5, 1: 6, 15: 7}

    def blocks_of(half, group):
        lines = [w[pl.ds(pl.multiple_of(half * 1024 + ((z + k) % NZ) * R, R), R), :] for k in group]
        return jnp.dot(jnp.concatenate(lines, axis=0), dl[...], preferred_element_type=F32)

    for i, group in enumerate(groups):
        xsend[i] = blocks_of(1 - xh, group).astype(BF16)
        send(xsend.at[i], xrecv.at[i], x_send.at[i], x_recv.at[i], across_x)
    climb(lrun, lgot, l_send, l_recv, 1)
    for i, group in enumerate(groups):
        own[i] = blocks_of(xh, group)
    links = iter(range(15))
    for i, group in enumerate(groups):
        arrived(xrecv.at[i], x_recv.at[i])
        both = own[i] + xrecv[i].astype(F32)
        own[i] = both
        zsend[i] = both.astype(BF16)
        for r, step in enumerate(group):
            piece = zsend.at[i, pl.ds(r * R, R)]
            if step in feeds:
                node, slot = feeds[step]
                send(piece, feed.at[slot], z_send.at[next(links)], f_recv.at[slot // 4], along_z(node))
            elif step not in (0, 4, 12):
                send(piece, zrecv.at[slots[step]], z_send.at[next(links)], z_recv, along_z(step))
        if i == 1:
            climb(lrun, lgot, l_send, l_recv, 2)
    for side, step, kept, count_in in ((1, 12, own[2, :R, :], 3), (0, 4, own[1, 3 * R :, :], 4)):
        arrived(feed.at[pl.ds(4 * side, count_in)], f_recv.at[side])
        for slot in range(count_in):
            kept = kept + feed[4 * side + slot].astype(F32)
        zagg[side] = kept.astype(BF16)
        send(zagg.at[side], zrecv.at[slots[step]], z_send.at[next(links)], z_recv, along_z(step))

    climb(lrun, lgot, l_send, l_recv, 3)
    kept = own[3, 3 * R :, :]
    arrived(zrecv, z_recv)
    for slot in range(8):
        kept = kept + zrecv[slot].astype(F32)
    grad_ref[...] = kept.astype(BF16)
    climb(lrun, lgot, l_send, l_recv, 4)
    loss = jnp.sum(lrun[4], axis=1, keepdims=True) / count
    row_ref[2:3] = jnp.broadcast_to(loss, (1, TOK))
    for copy in started:
        copy.wait_send()


def place(grad_in, row_in, grad_ref, kl_ref, samp_ref, loss_ref):
    grad_ref[...] = grad_in[...]
    kl_ref[...] = row_in[0]
    samp_ref[...] = row_in[1]
    loss_ref[...] = row_in[2:3, 0:1]


def on_device(hidden, blocks, teacher, ids, mask):
    vm = pl.BlockSpec(memory_space=pltpu.VMEM)
    hbm = pl.BlockSpec(memory_space=pl.ANY)
    dma = pltpu.SemaphoreType.DMA
    grad, rows = pl.pallas_call(
        kernel,
        out_shape=(jax.ShapeDtypeStruct((R, TOK), BF16), jax.ShapeDtypeStruct((8, TOK), F32)),
        in_specs=[hbm] * 5,
        out_specs=(vm, vm),
        scratch_shapes=[
            pltpu.VMEM((D, VT), BF16),
            pltpu.VMEM((NZ, 2 * R, TOK), BF16),
            pltpu.VMEM((4, TOK, 512), BF16),
            pltpu.VMEM((TOK, VT), F32),
            pltpu.VMEM((VT, TOK), F32),
            pltpu.VMEM((VT, TOK), F32),
            pltpu.VMEM((VT, TOK), F32),
            pltpu.VMEM((VT, TOK), BF16),
            pltpu.VMEM((32, 4, TOK), F32),
            pltpu.VMEM((32, 2, TOK), F32),
            pltpu.VMEM((R, VT), BF16),
            pltpu.VMEM((5, 1, TOK), F32),
            pltpu.VMEM((4, 1, TOK), F32),
            pltpu.VMEM((5, 1, TOK), F32),
            pltpu.VMEM((4, 1, TOK), F32),
            pltpu.VMEM((4, 256, TOK), BF16),
            pltpu.VMEM((4, 256, TOK), BF16),
            pltpu.VMEM((4, 256, TOK), F32),
            pltpu.VMEM((4, 256, TOK), BF16),
            pltpu.VMEM((8, R, TOK), BF16),
            pltpu.VMEM((7, R, TOK), BF16),
            pltpu.VMEM((2, R, TOK), BF16),
            pltpu.VMEM((TOK, VT), BF16),
            pltpu.VMEM((1, TOK), jnp.int32),
            pltpu.VMEM((1, TOK), jnp.int32),
            dma((48,)), dma((50,)), dma((48,)), dma((48,)), dma((6,)), dma((16,)), dma((4,)),
            dma((31,)), dma, dma((31,)), dma, dma((4,)), dma((4,)), dma((4,)), dma((4,)), dma((4,)), dma((4,)), dma((16,)), dma, dma((2,)),
            pltpu.SemaphoreType.REGULAR((4,)),
        ],
        compiler_params=pltpu.CompilerParams(
            collective_id=0, has_side_effects=True, vmem_limit_bytes=60 * 1024 * 1024
        ),
    )(hidden.T, blocks.reshape(R, 2 * VT), teacher, ids.reshape(1, TOK), mask.reshape(1, TOK))
    grad, kl, samp, loss = pl.pallas_call(
        place,
        out_shape=(
            jax.ShapeDtypeStruct((R, TOK), BF16),
            jax.ShapeDtypeStruct((TOK,), F32),
            jax.ShapeDtypeStruct((TOK,), F32),
            jax.ShapeDtypeStruct((1, 1), F32),
        ),
        in_specs=[vm, vm],
        out_specs=(vm, vm, vm, vm),
    )(grad, rows)
    return grad.T, kl, samp, loss.reshape(())


def solution(mesh):
    return jax.shard_map(
        on_device,
        mesh=mesh,
        in_specs=(P("dp", "vocab"), P("vocab", "dp", None), P("dp", "vocab"), P("dp"), P("dp")),
        out_specs=(P("dp", "vocab"), P("dp"), P("dp"), P()),
        check_vma=False,
    )
```
